32 devices in a mesh: gx: 4 (over z), gy: 4 (over y, x), gz: 2 (over core).
Axes of the slice: x: 2, y: 2, z: 4, core: 2. Of those that a mesh axis runs over, the one named last changes fastest.
Arguments:
- schur: bfloat16 [4, 4, 2, 2048, 2048], P('gx', 'gy', 'gz'), may hold values from -0.09375 to 0.09375
- interface_diag: float32 [4, 4, 2, 2048], P('gx', 'gy', 'gz'), may hold values from 2 to 4
- precond: float32 [4, 4, 2, 16, 128, 128], P('gx', 'gy', 'gz'), may hold values from -0.3 to 0.8
- load: bfloat16 [4, 4, 2, 2048, 256], P('gx', 'gy', 'gz'), may hold values from -170 to 170
- face_blocks: int32 [4, 4, 2, 6, 2], P('gx', 'gy', 'gz'), may hold values from 0 to 16, as said below
Outputs:
- solution: float32 [4, 4, 2, 2048, 256], P('gx', 'gy', 'gz')
- residual_norm: float32 [256], replicated
The draws below stay inside these ranges and needn't reach their ends.
Inputs may be any that keep to these rules, and one draw needn't show every extreme that they name: `face_blocks`: for each subdomain p and direction d (0, 1: next and previous along the first grid dimension; 2, 3 and 4, 5 likewise along the second and third), slots 0 to n - 1 hold block numbers below 16 shared with the neighbour in that direction, where n (1 to 2 inside the grid, 0 across its boundary) equals the neighbour's n for the opposite direction, and the neighbour's slot k of the opposite direction holds the block that shares with p's slot k; the remaining slots hold 16; no block number appears twice in one subdomain's table; some face shares 2 blocks in every draw.
All inputs are finite; a program needn't handle non-finite values.
Results may differ from the reference program's by a relative error of at most 0.0008.
Values sent between devices are 32-bit elements; how exact they have to be, the bound alone decides.
A program may use at most 128 MiB of HBM per device.

```python
import math
import jax
import jax.numpy as jnp
from jax import lax

BLK = 128
NBLK = 16
IFACE = 2048
CAP = 2
NRHS = 256
SUB_X = 4
SUB_Y = 4
SUB_Z = 2


def draw_precond(key, part):
    full_shape = (SUB_X, SUB_Y, SUB_Z, NBLK, BLK, BLK)
    key_diag, key_off = jax.random.split(jax.random.fold_in(key, 11))
    diagonal = 1.0 / jax.random.uniform(key_diag, full_shape[:-1], jnp.float32, 2.0, 4.0)
    coupling = jnp.clip(jax.random.normal(key_off, full_shape, jnp.float32), -6.0, 6.0) * (0.12 / math.sqrt(BLK))
    identity = jnp.eye(BLK, dtype=jnp.float32)
    return coupling + diagonal[..., None] * identity


def ramp_factor(length):
    return jnp.power(3.0, jnp.arange(length, dtype=jnp.float32) / max(length - 1, 1))


def draw_load(key, part):
    key_base = jax.random.fold_in(jax.random.fold_in(key, 5), 0)
    key_rows = jax.random.fold_in(jax.random.fold_in(key, 5), 2)
    key_cols = jax.random.fold_in(jax.random.fold_in(key, 5), 3)
    full_shape = (SUB_X, SUB_Y, SUB_Z, NBLK * BLK, NRHS)
    row_scale = jnp.exp(jax.random.uniform(key_rows, full_shape[:4] + (1,), jnp.float32, 0.0, math.log(10.0)))
    col_scale = jnp.exp(jax.random.uniform(key_cols, (NRHS,), jnp.float32, 0.0, math.log(10.0)))
    position = ramp_factor(SUB_X)[:, None, None] * ramp_factor(SUB_Y)[None, :, None] * ramp_factor(SUB_Z)[None, None, :]
    base = jnp.clip(jax.random.normal(key_base, full_shape, jnp.float32), -6.0, 6.0)
    values = 0.01 * base * row_scale * col_scale * position[..., None, None]
    return values.astype(jnp.bfloat16)


def pair_counts(pair_key, axis_id):
    grid_shape = [SUB_X, SUB_Y, SUB_Z]
    grid_shape[axis_id] = grid_shape[axis_id] - 1
    counts = jax.random.randint(pair_key, tuple(grid_shape), 1, CAP + 1, dtype=jnp.int32)
    if grid_shape[axis_id] > 0:
        counts = counts.at[0, 0, 0].set(CAP)
    pad_upper = [(0, 0)] * 3
    pad_upper[axis_id] = (0, 1)
    pad_lower = [(0, 0)] * 3
    pad_lower[axis_id] = (1, 0)
    return (jnp.pad(counts, pad_upper), jnp.pad(counts, pad_lower))


def draw_face_blocks(key, part):
    key_x, key_y, key_z, key_perm = jax.random.split(jax.random.fold_in(key, 7), 4)
    upper_x, lower_x = pair_counts(key_x, 0)
    upper_y, lower_y = pair_counts(key_y, 1)
    upper_z, lower_z = pair_counts(key_z, 2)
    dir_counts = jnp.stack([upper_x, lower_x, upper_y, lower_y, upper_z, lower_z], axis=-1)
    offsets = jnp.cumsum(dir_counts, axis=-1) - dir_counts
    subdomains = SUB_X * SUB_Y * SUB_Z
    perm_keys = jax.random.split(key_perm, subdomains)
    orders = jax.vmap(lambda one_key: jax.random.permutation(one_key, NBLK))(perm_keys).astype(jnp.int32)
    orders = orders.reshape(SUB_X, SUB_Y, SUB_Z, 1, NBLK)
    slot_ids = jnp.arange(CAP, dtype=jnp.int32)
    positions = jnp.minimum(offsets[..., None] + slot_ids, NBLK - 1).astype(jnp.int32)
    picked = jnp.take_along_axis(orders, positions.reshape(SUB_X, SUB_Y, SUB_Z, 1, 6 * CAP), axis=-1)
    picked = picked.reshape(SUB_X, SUB_Y, SUB_Z, 6, CAP)
    valid = slot_ids < dir_counts[..., None]
    return jnp.where(valid, picked, NBLK).astype(jnp.int32)


def block_levels(own_key, shape, pieces, least, top_value):
    gain = 1.0
    for dim, parts in pieces:
        draws = jax.random.uniform(jax.random.fold_in(jax.random.fold_in(own_key, 6), dim), (parts,), jnp.float32, least / len(pieces), top_value / len(pieces))
        gain = gain * jnp.repeat(jnp.exp(draws), shape[dim] // parts).reshape((-1,) + (1,) * (len(shape) - 1 - dim))
    return gain


def gaussian(stream_key, shape, width, reach, shards=(), kind=jnp.bfloat16):
    result = width * jax.random.normal(stream_key, shape, jnp.float32)
    if shards:
        result = result * block_levels(stream_key, shape, shards, -0.22, 0.18)
    return jnp.clip(result, -reach, reach).astype(kind)


def setup_inputs(seed: int = 0) -> dict:
    seeds = jax.random.split(jax.random.key(seed), 6)
    return {
        "schur": gaussian(seeds[0], (SUB_X, SUB_Y, SUB_Z, IFACE, IFACE), (2 * IFACE) ** -0.5, 0.09375, ((0, 4), (1, 4), (2, 2))),
        "interface_diag": jnp.clip(jnp.exp(math.log(4.0) - 0.6931472 * jax.random.uniform(seeds[1], (SUB_X, SUB_Y, SUB_Z, IFACE), jnp.float32) ** block_levels(seeds[1], (SUB_X, SUB_Y, SUB_Z, IFACE), ((0, 4), (1, 4), (2, 2)), -0.2, 0.2)), 2.0, 4.0),
        "precond": draw_precond(jax.random.fold_in(seeds[5], 71), 0),
        "load": draw_load(jax.random.fold_in(seeds[5], 71), 0),
        "face_blocks": draw_face_blocks(jax.random.fold_in(seeds[5], 71), 0),
    }


epsilon = 1e-06

def find_live(face_blocks):
    slot_hits = face_blocks[..., None] == jnp.arange(NBLK, dtype=jnp.int32)
    return jnp.any(slot_hits, axis=(3, 4)).astype(jnp.float32)

def from_next(values, axis_id):
    length = values.shape[axis_id]
    pad_spec = [(0, 0)] * values.ndim
    pad_spec[axis_id] = (0, 1)
    return lax.slice_in_dim(jnp.pad(values, pad_spec), 1, length + 1, axis=axis_id)

def from_prev(values, axis_id):
    length = values.shape[axis_id]
    pad_spec = [(0, 0)] * values.ndim
    pad_spec[axis_id] = (1, 0)
    return lax.slice_in_dim(jnp.pad(values, pad_spec), 0, length, axis=axis_id)

def assemble(blocks, face_blocks, live_mask):
    grid_shape = blocks.shape[:3]
    row_width = blocks.shape[-1]
    subdomains = grid_shape[0] * grid_shape[1] * grid_shape[2]
    flattened = blocks.reshape(subdomains, NBLK, BLK, row_width)
    extended = jnp.concatenate([flattened, jnp.zeros((subdomains, 1, BLK, row_width), jnp.float32)], axis=1)
    slot_index = face_blocks.reshape(subdomains, 6 * CAP).astype(jnp.int32)
    packed = jax.vmap(lambda table, picks: table[picks])(extended, slot_index)
    packed = packed.reshape(grid_shape + (6, CAP, BLK, row_width))
    arrived = jnp.stack([from_next(packed[:, :, :, 1], 0), from_prev(packed[:, :, :, 0], 0), from_next(packed[:, :, :, 3], 1), from_prev(packed[:, :, :, 2], 1), from_next(packed[:, :, :, 5], 2), from_prev(packed[:, :, :, 4], 2)], axis=3)
    arrived = arrived.reshape(subdomains, 6 * CAP, BLK, row_width)
    extended = jax.vmap(lambda table, picks, extra: table.at[picks].add(extra))(extended, slot_index, arrived)
    return extended[:, :NBLK].reshape(blocks.shape) * live_mask[..., None, None]

def inner_product(left_vec, right_vec):
    return 0.5 * lax.optimization_barrier(jnp.sum(left_vec * right_vec, axis=(0, 1, 2, 3, 4)))

def precondition(vector, precond, face_blocks, live_mask):
    partial_value = jnp.einsum('xyzbij,xyzbjr->xyzbir', precond, vector, precision=lax.Precision.HIGHEST)
    return assemble(partial_value, face_blocks, live_mask)

def operate(vector, schur, interface_diag, face_blocks, live_mask):
    subdomains = SUB_X * SUB_Y * SUB_Z
    flat_schur = schur.reshape(subdomains, IFACE, IFACE)
    flat_vector = vector.reshape(subdomains, IFACE, NRHS)
    product = lax.map(lambda pair: jnp.dot(pair[0], pair[1].astype(jnp.bfloat16), preferred_element_type=jnp.float32), (flat_schur, flat_vector))
    partial_value = product + interface_diag.reshape(subdomains, IFACE, 1) * flat_vector
    return assemble(partial_value.reshape(vector.shape), face_blocks, live_mask)

def reference(schur, interface_diag, precond, load, face_blocks):
    live_mask = find_live(face_blocks)
    block_shape = (SUB_X, SUB_Y, SUB_Z, NBLK, BLK, NRHS)
    assembled_load = assemble(load.astype(jnp.float32).reshape(block_shape), face_blocks, live_mask)
    initial = jnp.sqrt(inner_product(assembled_load, assembled_load) + epsilon)
    basis_first = assembled_load / initial
    precond_first = precondition(basis_first, precond, face_blocks, live_mask)
    working = operate(precond_first, schur, interface_diag, face_blocks, live_mask)
    diag_first = inner_product(working, basis_first)
    working = working - diag_first * basis_first
    below_first = jnp.sqrt(inner_product(working, working) + epsilon)
    basis_second = working / below_first
    precond_second = precondition(basis_second, precond, face_blocks, live_mask)
    working = operate(precond_second, schur, interface_diag, face_blocks, live_mask)
    upper_second = inner_product(working, basis_first)
    working = working - upper_second * basis_first
    diag_second = inner_product(working, basis_second)
    working = working - diag_second * basis_second
    below_second = jnp.sqrt(inner_product(working, working) + epsilon)
    radius_first = jnp.sqrt(diag_first * diag_first + below_first * below_first)
    cosine_first = diag_first / radius_first
    sine_first = below_first / radius_first
    rotated_top = cosine_first * upper_second + sine_first * diag_second
    rotated_low = cosine_first * diag_second - sine_first * upper_second
    radius_second = jnp.sqrt(rotated_low * rotated_low + below_second * below_second)
    cosine_second = rotated_low / radius_second
    sine_second = below_second / radius_second
    weight_second = -initial * sine_first * cosine_second / radius_second
    weight_first = (initial * cosine_first - rotated_top * weight_second) / radius_first
    solution = weight_first * precond_first + weight_second * precond_second
    residual_norm = initial * sine_first * sine_second
    return (solution.reshape(SUB_X, SUB_Y, SUB_Z, IFACE, NRHS), residual_norm)
```

```python
import functools

import jax
import jax.numpy as jnp
from jax import lax
from jax.experimental import pallas as pl
from jax.experimental.pallas import tpu as pltpu
from jax.sharding import PartitionSpec as P

EPS = 1e-06
MESH = pl.DeviceIdType.MESH
AXES = ("gx", "gy", "gz")
LANES = 128
F32 = jnp.float32
BF16 = jnp.bfloat16
ORDER = (2, 3, 0, 1, 4, 5)
NEAR = (4, 5, 0, 1)
FAR = (2, 3)


def kernel(
    sizes,
    table_hbm,
    schur_hbm,
    diag_hbm,
    prec_hbm,
    load_hbm,
    z1_ref,
    z2_ref,
    final_ref,
    table,
    load_all,
    prec_all,
    diag_all,
    schur_all,
    schur_slots,
    diag_slots,
    load_send,
    load_recv,
    prec_send,
    prec_recv,
    prec_split,
    rhs,
    q_ref,
    u1_send,
    u1_recv,
    u2_send,
    u2_recv,
    pass_full,
    pass_half,
    sums,
    plane_one,
    line_one,
    plane_two,
    line_two,
    local_sems,
    face_send,
    face_recv,
    pass_send,
    pass_recv,
    plane_send,
    plane_recv,
    line_send,
    line_recv,
):
    nx, ny, nz = sizes
    planes = ny * nz
    groups, _, rows, lanes = load_send.shape
    nblk, blk = prec_hbm.shape[:2]
    cap = rows // blk
    slots = 6 * cap
    half = rows // 2
    gx, gy, gz = (lax.axis_index(a) for a in AXES)
    here = gy * nz + gz
    relayed = ny == 4 and nz == 2

    moves = [(table_hbm, table), (load_hbm, load_all), (prec_hbm, prec_all), (diag_hbm, diag_all)]
    for b in range(nblk):
        moves.append((schur_hbm.at[:, :, pl.ds(b * blk, blk)], schur_all.at[b]))
    local = [
        pltpu.make_async_copy(source, target, local_sems.at[i])
        for i, (source, target) in enumerate(moves)
    ]
    for copy in local:
        copy.start()

    def plane_peer(step):
        other = lax.rem(here + step, planes)
        return (gx, other // nz, lax.rem(other, nz))

    def line_peer(step):
        return (lax.rem(gx + step, nx), gy, gz)

    barrier = pltpu.get_barrier_semaphore()
    for step in range(1, planes):
        pl.semaphore_signal(barrier, inc=1, device_id=plane_peer(step), device_id_type=MESH)
    for step in range(1, nx):
        pl.semaphore_signal(barrier, inc=1, device_id=line_peer(step), device_id_type=MESH)

    target, has = [], []
    for d in range(6):
        at = [gx, gy, gz]
        if d % 2 == 0:
            has.append(at[d // 2] + 1 < sizes[d // 2])
            at[d // 2] = at[d // 2] + 1
        else:
            has.append(at[d // 2] > 0)
            at[d // 2] = at[d // 2] - 1
        target.append(tuple(at))

    def message(kind, g=0):
        number = {"load": g, "prec": groups, "one": groups + 1 + g, "two": 2 * groups + 1 + g}[kind]
        if kind == "load":
            return number, load_send.at[g], load_recv.at[g], pass_full.at[number], rows, 0
        if kind == "prec":
            return number, prec_send, prec_recv, pass_full.at[number], rows, 0
        if kind == "one":
            return number, u1_send.at[g], u1_recv.at[g], pass_full.at[number], rows, 0
        return number, u2_send.at[g], u2_recv.at[g], pass_half.at[g], half, half

    def parts(d):
        return 2 if relayed and d in FAR else 1

    def sem_of(d, h):
        return 2 * d + h

    def face(msg, d, h, slot, device):
        number, source, landing, _, count, shift = msg
        n = parts(d)
        size = count // n
        begin = (shift if d % 2 == 0 else 0) + h * size
        return pltpu.make_async_remote_copy(
            src_ref=source.at[d, pl.ds(begin, size)],
            dst_ref=landing.at[slot, pl.ds(h * size, size)],
            send_sem=face_send.at[number, sem_of(d, h)],
            recv_sem=face_recv.at[number, sem_of(slot, h)],
            device_id=device,
            device_id_type=MESH,
        )

    def ends(d):
        return (1, 3, 2) if d == 2 else (2, 0, 1)

    def send(msg, d):
        number, source, _, middle, count, shift = msg

        @pl.when(has[d])
        def _():
            if parts(d) == 2:
                first, via, _ = ends(d)
                size = count // 2
                begin = (shift if d % 2 == 0 else 0) + size

                @pl.when(gy == first)
                def _():
                    pltpu.make_async_remote_copy(
                        src_ref=source.at[d, pl.ds(begin, size)],
                        dst_ref=middle,
                        send_sem=face_send.at[number, sem_of(d, 1)],
                        recv_sem=pass_recv.at[number],
                        device_id=(gx, via, gz),
                        device_id_type=MESH,
                    ).start()

                @pl.when(gy != first)
                def _():
                    face(msg, d, 1, d ^ 1, target[d]).start()

            face(msg, d, 0, d ^ 1, target[d]).start()

    def forward(msg, d):
        number, _, landing, middle, count, _ = msg
        size = count // 2
        return pltpu.make_async_remote_copy(
            src_ref=middle,
            dst_ref=landing.at[d ^ 1, pl.ds(size, size)],
            send_sem=pass_send.at[number],
            recv_sem=face_recv.at[number, sem_of(d ^ 1, 1)],
            device_id=(gx, ends(d)[2], gz),
            device_id_type=MESH,
        )

    def relay(msg):
        if not relayed:
            return
        number, _, _, middle, _, _ = msg
        for d in FAR:
            @pl.when(gy == ends(d)[1])
            def _(d=d):
                pltpu.make_async_remote_copy(
                    src_ref=middle,
                    dst_ref=middle,
                    send_sem=pass_send.at[number],
                    recv_sem=pass_recv.at[number],
                    device_id=(gx, ends(d)[0], gz),
                    device_id_type=MESH,
                ).wait_recv()
                forward(msg, d).start()

    def arrived(msg, d):
        for h in range(parts(d)):
            face(msg, d, h, d, target[d]).wait_recv()

    def all_sent(msg):
        for d in range(6):
            @pl.when(has[d])
            def _(d=d):
                for h in range(parts(d)):
                    face(msg, d, h, d ^ 1, target[d]).wait_send()

        if relayed:
            for d in FAR:
                @pl.when(gy == ends(d)[1])
                def _(d=d):
                    forward(msg, d).wait_send()

    def reduce_copy(number, buf, step, slot, me, peer, send_sem, recv_sem):
        return pltpu.make_async_remote_copy(
            src_ref=buf.at[me],
            dst_ref=buf.at[slot],
            send_sem=send_sem.at[number, step - 1],
            recv_sem=recv_sem.at[number, step - 1],
            device_id=peer(step),
            device_id_type=MESH,
        )

    def reduce_start(number, buf, count, me, peer, send_sem, recv_sem):
        for step in range(1, count):
            reduce_copy(number, buf, step, me, me, peer, send_sem, recv_sem).start()

    def reduce_wait(number, buf, count, me, peer, send_sem, recv_sem, sent):
        for step in range(1, count):
            came = me if sent else lax.rem(me + count - step, count)
            copy = reduce_copy(number, buf, step, came, me, peer, send_sem, recv_sem)
            if sent:
                copy.wait_send()
            else:
                copy.wait_recv()

    plane_args = (planes, here, plane_peer, plane_send, plane_recv)
    line_args = (nx, gx, line_peer, line_send, line_recv)

    def plane_of(number):
        return plane_one.at[number] if number < groups else plane_two

    def line_of(number):
        return line_one.at[number] if number < groups else line_two

    def total_of(buf, count):
        total = buf[0]
        for i in range(1, count):
            total = total + buf[i]
        return total

    def reduce_middle(number):
        reduce_wait(number, plane_of(number), *plane_args, False)
        line_of(number)[gx] = total_of(plane_of(number), planes)
        reduce_start(number, line_of(number), *line_args)

    def reduce_end(number):
        reduce_wait(number, line_of(number), *line_args, False)
        return total_of(line_of(number), nx)

    def folded(x):
        return jnp.sum(x.reshape(x.shape[0] // 8, 8, lanes), axis=0)

    def add_sum(g, i, x):
        sums[g, i] = sums[g, i] + x

    local[0].wait()
    picks = [table[s % cap, s // cap] for s in range(slots)]
    index = [jnp.minimum(p, nblk - 1) for p in picks]
    mask = [jnp.minimum(nblk - p, 1).astype(F32) for p in picks]

    def gather_load(g, d):
        for k in range(cap):
            s = d * cap + k
            value = load_all[index[s], :, g * lanes : (g + 1) * lanes].astype(F32)
            load_send[g, d, k * blk : (k + 1) * blk] = value * mask[s]

    def gather_prec(d):
        for k in range(cap):
            prec_send[d, k * blk : (k + 1) * blk] = prec_all[index[d * cap + k]]

    local[1].wait()
    gather_load(0, 2)
    gather_load(0, 3)
    pl.semaphore_wait(barrier, planes - 1 + nx - 1)
    load_0 = message("load", 0)
    prec = message("prec")
    send(load_0, 2)
    gather_load(0, 0)
    send(load_0, 3)
    gather_load(0, 1)
    send(load_0, 0)
    gather_load(0, 4)
    send(load_0, 1)
    gather_load(0, 5)
    send(load_0, 4)
    local[2].wait()
    gather_prec(2)
    send(load_0, 5)
    gather_prec(3)
    send(prec, 2)
    gather_prec(0)
    send(prec, 3)
    gather_prec(1)
    send(prec, 0)
    gather_prec(4)
    send(prec, 1)
    gather_prec(5)
    send(prec, 4)
    for g in range(1, groups):
        for d in range(6):
            gather_load(g, d)
    send(prec, 5)
    sums[...] = jnp.zeros(sums.shape, F32)
    u1_send[...] = jnp.zeros(u1_send.shape, F32)
    u2_send[...] = jnp.zeros(u2_send.shape, F32)
    relay(load_0)
    relay(prec)
    for g in range(1, groups):
        for d in ORDER:
            send(message("load", g), d)

    local[3].wait()
    eye = lax.broadcasted_iota(jnp.int32, (blk, blk), 0) == lax.broadcasted_iota(
        jnp.int32, (blk, blk), 1
    )
    for s in range(slots):
        column = jnp.sum(jnp.where(eye, diag_all[index[s]], 0.0), axis=1, keepdims=True)
        diag_slots[s * blk : (s + 1) * blk] = jnp.broadcast_to(column, (blk, lanes))
    for copy in local[4:]:
        copy.wait()
    for s in range(slots):
        for t in range(slots):
            tile = schur_all[index[t], index[s]]
            schur_slots[s * blk : (s + 1) * blk, t * blk : (t + 1) * blk] = tile
    for g in range(1, groups):
        relay(message("load", g))

    def precondition(s, value):
        high = value.astype(BF16)
        low = (value - high.astype(F32)).astype(BF16)
        top = jnp.concatenate([high, low], axis=1)
        bottom = jnp.concatenate([high, jnp.zeros_like(low)], axis=1)
        z = jnp.dot(
            prec_split[s], jnp.concatenate([top, bottom], axis=0), preferred_element_type=F32
        )
        return z[:, :lanes] + z[:, lanes:]

    def multiply(d, z, into):
        narrow = jnp.concatenate([part.astype(BF16) for part in z], axis=0)
        product = jnp.dot(
            schur_slots[:, d * rows : (d + 1) * rows], narrow, preferred_element_type=F32
        )
        into[...] = into[...] + product.reshape(6, rows, lanes)

    def first_step(g, d):
        @pl.when(has[d])
        def _():
            arrived(message("load", g), d)
            if g == 0:
                arrived(prec, d)
                for k in range(cap):
                    at = slice(k * blk, (k + 1) * blk)
                    block = prec_send[d, at] + prec_recv[d, at]
                    high = block.astype(BF16)
                    low = (block - high.astype(F32)).astype(BF16)
                    prec_split[d * cap + k] = jnp.concatenate([high, low], axis=1)
            z = []
            square = jnp.zeros((8, lanes), F32)
            for k in range(cap):
                at = slice(k * blk, (k + 1) * blk)
                value = load_send[g, d, at] + load_recv[g, d, at]
                rhs[g, d, at] = value
                square = square + folded(value * value)
                z.append(precondition(d * cap + k, value))
                z1_ref[g, d * cap + k] = z[-1]
            add_sum(g, 0, square)
            multiply(d, z, u1_send.at[g])

    def first_done(g):
        for d in ORDER:
            @pl.when(has[d])
            def _(d=d):
                scale = diag_slots[d * rows : (d + 1) * rows]
                z = z1_ref[g, d * cap : (d + 1) * cap].reshape(rows, lanes)
                value = u1_send[g, d] + scale * z
                u1_send[g, d] = value
                add_sum(g, 1, folded(value * rhs[g, d]))

    def pack(values):
        return jnp.concatenate([jnp.sum(v, axis=0, keepdims=True) for v in values], axis=0)

    for g in range(groups):
        for d in NEAR:
            first_step(g, d)
        if g:
            reduce_middle(g - 1)
            relay(message("one", g - 1))
        for d in FAR:
            first_step(g, d)
        first_done(g)
        plane_one[g, here] = pack((0.5 * sums[g, 0], sums[g, 1]))
        reduce_start(g, plane_one.at[g], *plane_args)
        for d in ORDER:
            send(message("one", g), d)

    def second_step(g, d, h11):
        @pl.when(has[d])
        def _():
            arrived(message("one", g), d)
            z = []
            square = jnp.zeros((8, lanes), F32)
            for k in range(cap):
                s = d * cap + k
                at = slice(k * blk, (k + 1) * blk)
                w = (u1_send[g, d, at] + u1_recv[g, d, at]) * mask[s]
                value = w - h11 * rhs[g, d, at]
                q_ref[g, d, at] = value
                square = square + folded(value * value)
                z.append(precondition(s, value))
                z2_ref[g, s] = z[-1]
            add_sum(g, 2, square)
            multiply(d, z, u2_send.at[g])

    def second_done(g):
        for i, d in enumerate(ORDER):
            @pl.when(has[d])
            def _(d=d):
                scale = diag_slots[d * rows : (d + 1) * rows]
                z = z2_ref[g, d * cap : (d + 1) * cap].reshape(rows, lanes)
                value = u2_send[g, d] + scale * z
                u2_send[g, d] = value
                add_sum(g, 3, folded(value * rhs[g, d]))
                add_sum(g, 4, folded(value * q_ref[g, d]))

            if i:
                send(message("two", g), ORDER[i - 1])
        send(message("two", g), ORDER[-1])

    def third_step(g, d):
        @pl.when(has[d])
        def _():
            arrived(message("two", g), d)
            begin = 0 if d % 2 == 0 else half
            work = jnp.zeros((8, lanes), F32)
            size = min(half, blk)
            for row in range(0, half, size):
                w = u2_send[g, d, begin + row : begin + row + size]
                w = (w + u2_recv[g, d, row : row + size]) * mask[d * cap + (begin + row) // blk]
                work = work + folded(w * w)
            add_sum(g, 5, work)

    if groups == 1:
        reduce_middle(0)
        relay(message("one", 0))
    squares, inners = [], []
    for g in range(groups):
        total = reduce_end(g)
        squares.append(total[0:1])
        inners.append(total[1:2] / (total[0:1] + EPS))
        for d in NEAR:
            second_step(g, d, inners[g])
        if g == 0 and groups > 1:
            reduce_middle(groups - 1)
            relay(message("one", groups - 1))
        if g:
            relay(message("two", g - 1))
        for d in FAR:
            second_step(g, d, inners[g])
        second_done(g)

    for g in range(groups):
        for d in NEAR:
            third_step(g, d)
        if g == 0:
            relay(message("two", groups - 1))
        for d in FAR:
            third_step(g, d)

    packed = []
    for g in range(groups):
        packed.append(pack((0.5 * sums[g, 2], sums[g, 3], sums[g, 4], sums[g, 5])))
    plane_two[here] = jnp.concatenate(packed, axis=0)
    reduce_start(groups, plane_two, *plane_args)
    reduce_middle(groups)
    total = reduce_end(groups)
    for g in range(groups):
        q_square, first, second, work = (total[4 * g + i : 4 * g + i + 1] for i in range(4))
        load_square, h11 = squares[g], inners[g]
        beta = jnp.sqrt(load_square + EPS)
        inverse = 1.0 / beta
        h21 = jnp.sqrt(q_square * inverse * inverse + EPS)
        t = inverse / h21
        h12 = first * t * inverse
        a22 = second * t * t
        ww = work * t * t
        n1 = load_square * inverse * inverse
        n2 = q_square * t * t
        g12 = h11 * EPS * inverse * t
        h22 = a22 - h12 * g12
        left = (
            ww
            - h12 * h12 * (2.0 - n1)
            - h22 * (2.0 * a22 - h22 * n2)
            + 2.0 * h12 * h22 * g12
        )
        h32 = jnp.sqrt(jnp.maximum(left, 0.0) + EPS)
        r1 = jnp.sqrt(h11 * h11 + h21 * h21)
        c1 = h11 / r1
        s1 = h21 / r1
        top = c1 * h12 + s1 * h22
        low = c1 * h22 - s1 * h12
        r2 = jnp.sqrt(low * low + h32 * h32)
        c2 = low / r2
        s2 = h32 / r2
        y2 = -beta * s1 * c2 / r2
        y1 = (beta * c1 - top * y2) / r1
        final_ref[3 * g : 3 * g + 1] = y1 * inverse
        final_ref[3 * g + 1 : 3 * g + 2] = y2 * t
        final_ref[3 * g + 2 : 3 * g + 3] = beta * s1 * s2

    for g in range(groups):
        for kind in ("load", "one", "two"):
            all_sent(message(kind, g))
    all_sent(prec)
    for number in range(groups + 1):
        reduce_wait(number, plane_of(number), *plane_args, True)
        reduce_wait(number, line_of(number), *line_args, True)


def place(table_hbm, z1, z2, final, out_ref, norm_ref, buf, norm_buf, table, sems, table_sem):
    groups, slots = z1.shape[:2]
    lanes = z1.shape[-1]
    nblk = out_ref.shape[0]
    cap = slots // 6
    for g in range(groups):
        norm_buf[:, g * lanes : (g + 1) * lanes] = final[3 * g + 2 : 3 * g + 3]
    move = pltpu.make_async_copy(table_hbm, table, table_sem)
    move.start()
    copies = [pltpu.make_async_copy(norm_buf, norm_ref, sems.at[nblk])]
    copies[0].start()
    move.wait()
    picks = [table[s % cap, s // cap] for s in range(slots)]
    for b in range(nblk):
        found = jnp.int32(slots)
        for s in range(slots):
            found = jnp.where(picks[s] == b, jnp.int32(s), found)
        at = jnp.minimum(found, slots - 1)
        for g in range(groups):
            value = final[3 * g : 3 * g + 1] * z1[g, at] + final[3 * g + 1 : 3 * g + 2] * z2[g, at]
            buf[b, :, g * lanes : (g + 1) * lanes] = jnp.where(found < slots, value, 0.0)
        copies.append(pltpu.make_async_copy(buf.at[b], out_ref.at[b], sems.at[b]))
        copies[-1].start()
    for copy in copies:
        copy.wait()


def in_hbm(x):
    return pltpu.with_memory_space_constraint(x, pltpu.HBM)


def on_device(sizes, schur, interface_diag, precond, load, face_blocks):
    nblk, blk = precond.shape[3:5]
    cols = load.shape[-1]
    order = schur.shape[-1]
    cap = face_blocks.shape[-1]
    slots = 6 * cap
    rows = cap * blk
    nx, ny, nz = sizes
    planes = ny * nz
    groups = cols // LANES
    messages = 3 * groups + 1
    vmem = pltpu.VMEM
    dma = pltpu.SemaphoreType.DMA
    hbm = pl.BlockSpec(memory_space=pltpu.HBM)
    local = pl.BlockSpec(memory_space=pltpu.VMEM)
    scalars = pl.BlockSpec(memory_space=pltpu.SMEM)
    table = face_blocks.reshape(6, cap).T
    mib = 1024 * 1024
    z1, z2, final = pl.pallas_call(
        functools.partial(kernel, sizes),
        out_shape=(
            jax.ShapeDtypeStruct((groups, slots, blk, LANES), F32),
            jax.ShapeDtypeStruct((groups, slots, blk, LANES), F32),
            jax.ShapeDtypeStruct((3 * groups, LANES), F32),
        ),
        in_specs=[hbm] * 5,
        out_specs=(local,) * 3,
        scratch_shapes=[
            pltpu.SMEM((cap, 6), jnp.int32),
            vmem((nblk, blk, cols), BF16),
            vmem((nblk, blk, blk), F32),
            vmem((nblk, 1, blk), F32),
            vmem((nblk, nblk, blk, blk), BF16),
            vmem((slots * blk, slots * blk), BF16),
            vmem((slots * blk, LANES), F32),
            vmem((groups, 6, rows, LANES), F32),
            vmem((groups, 6, rows, LANES), F32),
            vmem((6, rows, blk), F32),
            vmem((6, rows, blk), F32),
            vmem((slots, blk, 2 * blk), BF16),
            vmem((groups, 6, rows, LANES), F32),
            vmem((groups, 6, rows, LANES), F32),
            vmem((groups, 6, rows, LANES), F32),
            vmem((groups, 6, rows, LANES), F32),
            vmem((groups, 6, rows, LANES), F32),
            vmem((groups, 6, rows // 2, LANES), F32),
            vmem((2 * groups + 1, rows // 2, LANES), F32),
            vmem((groups, rows // 4, LANES), F32),
            vmem((groups, 6, 8, LANES), F32),
            vmem((groups, planes, 2, LANES), F32),
            vmem((groups, nx, 2, LANES), F32),
            vmem((planes, 4 * groups, LANES), F32),
            vmem((nx, 4 * groups, LANES), F32),
            dma((4 + nblk,)),
            dma((messages, 12)),
            dma((messages, 12)),
            dma((messages,)),
            dma((messages,)),
            dma((groups + 1, max(planes - 1, 1))),
            dma((groups + 1, max(planes - 1, 1))),
            dma((groups + 1, max(nx - 1, 1))),
            dma((groups + 1, max(nx - 1, 1))),
        ],
        compiler_params=pltpu.CompilerParams(
            collective_id=0, has_side_effects=True, vmem_limit_bytes=48 * mib
        ),
    )(
        in_hbm(table),
        in_hbm(schur.reshape(nblk, blk, order)),
        in_hbm(interface_diag.reshape(nblk, 1, blk)),
        in_hbm(precond.reshape(nblk, blk, blk)),
        in_hbm(load.reshape(nblk, blk, cols)),
    )
    result, norm = pl.pallas_call(
        place,
        out_shape=(
            jax.ShapeDtypeStruct((nblk, blk, cols), F32),
            jax.ShapeDtypeStruct((1, cols), F32),
        ),
        in_specs=[hbm, local, local, local],
        out_specs=(hbm, hbm),
        scratch_shapes=[vmem((nblk, blk, cols), F32), vmem((1, cols), F32), pltpu.SMEM((cap, 6), jnp.int32), dma((nblk + 1,)), dma(())],
        compiler_params=pltpu.CompilerParams(vmem_limit_bytes=16 * mib),
    )(in_hbm(table), z1, z2, final)
    return result.reshape(1, 1, 1, nblk * blk, cols), norm.reshape(cols)


def solution(mesh):
    sizes = tuple(mesh.shape[a] for a in AXES)
    placed = (
        P("gx", "gy", "gz", None, None),
        P("gx", "gy", "gz", None),
        P("gx", "gy", "gz", None, None, None),
        P("gx", "gy", "gz", None, None),
        P("gx", "gy", "gz", None, None),
    )
    return jax.shard_map(
        functools.partial(on_device, sizes),
        mesh=mesh,
        in_specs=placed,
        out_specs=(P("gx", "gy", "gz", None, None), P()),
        check_vma=False,
    )
```

```python
import functools

import jax
import jax.numpy as jnp
from jax import lax
from jax.experimental import pallas as pl
from jax.experimental.pallas import tpu as pltpu
from jax.sharding import PartitionSpec as P

EPS = 1e-06
MESH = pl.DeviceIdType.MESH
AXES = ("gx", "gy", "gz")
LANES = 128
F32 = jnp.float32
BF16 = jnp.bfloat16
ORDER = (2, 3, 0, 1, 4, 5)
NEAR = (4, 5, 0, 1)
FAR = (2, 3)
ALL = (0, 1, 2, 3, 4, 5)


def kernel(
    sizes,
    table_hbm,
    schur_hbm,
    diag_hbm,
    prec_hbm,
    load_hbm,
    z1_out,
    z2_out,
    final_ref,
    table,
    load_all,
    prec_all,
    diag_all,
    schur_all,
    schur_slots,
    diag_slots,
    first_send,
    first_recv,
    load_send,
    load_recv,
    prec_split,
    rhs,
    a_ref,
    z1_ref,
    z2_ref,
    u1_send,
    u1_recv,
    u2_send,
    u2_recv,
    pass_first,
    pass_full,
    pass_half,
    pass_last,
    sums,
    plane_one,
    line_one,
    plane_two,
    line_two,
    local_sems,
    face_send,
    face_recv,
    pass_send,
    pass_recv,
    plane_send,
    plane_recv,
    line_send,
    line_recv,
):
    nx, ny, nz = sizes
    planes = ny * nz
    groups, _, rows, lanes = rhs.shape
    nblk, blk = prec_hbm.shape[:2]
    cap = rows // blk
    slots = 6 * cap
    half = rows // 2
    gx, gy, gz = (lax.axis_index(a) for a in AXES)
    here = gy * nz + gz
    relayed = ny == 4 and nz == 2

    moves = [(table_hbm, table), (load_hbm, load_all), (prec_hbm, prec_all), (diag_hbm, diag_all)]
    local = [
        pltpu.make_async_copy(source, target, local_sems.at[i])
        for i, (source, target) in enumerate(moves)
    ]
    for copy in local:
        copy.start()
    for b in range(nblk):
        pltpu.make_async_copy(
            schur_hbm.at[:, :, pl.ds(b * blk, blk)], schur_all.at[b], local_sems.at[4]
        ).start()

    def plane_peer(step):
        other = lax.rem(here + step, planes)
        return (gx, other // nz, lax.rem(other, nz))

    def line_peer(step):
        return (lax.rem(gx + step, nx), gy, gz)

    target, has = [], []
    for d in range(6):
        at = [gx, gy, gz]
        if d % 2 == 0:
            has.append(at[d // 2] + 1 < sizes[d // 2])
            at[d // 2] = at[d // 2] + 1
        else:
            has.append(at[d // 2] > 0)
            at[d // 2] = at[d // 2] - 1
        target.append(tuple(at))

    barrier = pltpu.get_barrier_semaphore()
    near = relayed and nx <= 4
    entered = jnp.int32(1)
    if near:
        for d in range(6):
            entered = entered + has[d].astype(jnp.int32)

            @pl.when(has[d])
            def _(d=d):
                pl.semaphore_signal(barrier, inc=1, device_id=target[d], device_id_type=MESH)

        pl.semaphore_signal(
            barrier, inc=1, device_id=(gx, lax.rem(gy + 2, ny), gz), device_id_type=MESH
        )
    else:
        entered = planes - 1 + nx - 1
        for step in range(1, planes):
            pl.semaphore_signal(barrier, inc=1, device_id=plane_peer(step), device_id_type=MESH)
        for step in range(1, nx):
            pl.semaphore_signal(barrier, inc=1, device_id=line_peer(step), device_id_type=MESH)

    def message(kind, g):
        if kind == "load" and g == 0:
            return g, g, first_send, first_recv, pass_first, 2 * rows, 0, rows
        if kind == "load":
            return g, g, load_send.at[g - 1], load_recv.at[g - 1], pass_full.at[g - 1], rows, 0, half
        if kind == "one":
            middle = pass_full.at[groups - 1 + g]
            return g, groups + g, u1_send.at[g], u1_recv.at[g], middle, rows, 0, half
        if g == groups - 1:
            return g, g, u2_send.at[g], u2_recv.at[g], pass_last, half, half, half // 4
        return g, g, u2_send.at[g], u2_recv.at[g], pass_half.at[g], half, half, half // 2

    def before(kind, g):
        return {"load": None, "one": ("load", g), "two": ("one", g)}[kind]

    def ends(d):
        return (1, 3, 2) if d == 2 else (2, 0, 1)

    def face(msg, d, slot, device, row=0, size=None):
        g, number, source, landing, _, count, shift, _ = msg
        size = size or count
        begin = (shift if d % 2 == 0 else 0) + row
        return pltpu.make_async_remote_copy(
            src_ref=source.at[d, pl.ds(begin, size)],
            dst_ref=landing.at[slot, pl.ds(row, size)],
            send_sem=face_send.at[g, d],
            recv_sem=face_recv.at[number, slot],
            device_id=device,
            device_id_type=MESH,
        )

    def to_relay(msg, d):
        g, number, source, _, middle, count, shift, via = msg
        begin = (shift if d % 2 == 0 else 0) + count - via
        return pltpu.make_async_remote_copy(
            src_ref=source.at[d, pl.ds(begin, via)],
            dst_ref=middle,
            send_sem=face_send.at[g, d],
            recv_sem=pass_recv.at[number],
            device_id=(gx, ends(d)[1], gz),
            device_id_type=MESH,
        )

    def sent(msg, d):
        face(msg, d, d ^ 1, target[d]).wait_send()

    def send(kind, g, d):
        msg = message(kind, g)
        count, via = msg[5], msg[7]

        @pl.when(has[d])
        def _():
            if before(kind, g):
                sent(message(*before(kind, g)), d)
            if relayed and d in FAR:
                @pl.when(gy == ends(d)[0])
                def _():
                    to_relay(msg, d).start()
                    face(msg, d, d ^ 1, target[d], 0, count - via).start()

                @pl.when(gy != ends(d)[0])
                def _():
                    face(msg, d, d ^ 1, target[d]).start()
            else:
                face(msg, d, d ^ 1, target[d]).start()

    def forward(msg, d):
        g, number, _, landing, middle, count, _, via = msg
        return pltpu.make_async_remote_copy(
            src_ref=middle,
            dst_ref=landing.at[d ^ 1, pl.ds(count - via, via)],
            send_sem=pass_send.at[g],
            recv_sem=face_recv.at[number, d ^ 1],
            device_id=(gx, ends(d)[2], gz),
            device_id_type=MESH,
        )

    def relay(kind, g):
        if not relayed:
            return
        msg = message(kind, g)
        for d in FAR:
            @pl.when(gy == ends(d)[1])
            def _(d=d):
                to_relay(msg, d).wait_recv()
                if before(kind, g):
                    forward(message(*before(kind, g)), d).wait_send()
                forward(msg, d).start()

    def arrived(kind, g, d):
        face(message(kind, g), d, d, target[d]).wait_recv()

    def all_sent(kind, g):
        msg = message(kind, g)
        for d in range(6):
            @pl.when(has[d])
            def _(d=d):
                sent(msg, d)

        if relayed:
            for d in FAR:
                @pl.when(gy == ends(d)[1])
                def _(d=d):
                    forward(msg, d).wait_send()

    def reduce_start(number, buf, count, me, peer, send_sem, recv_sem):
        for step in range(1, count):
            pltpu.make_async_remote_copy(
                src_ref=buf.at[me],
                dst_ref=buf.at[me],
                send_sem=send_sem.at[number],
                recv_sem=recv_sem.at[number],
                device_id=peer(step),
                device_id_type=MESH,
            ).start()

    def reduce_wait(number, buf, count, me, peer, send_sem, recv_sem, sent):
        if count > 1:
            copy = pltpu.make_async_remote_copy(
                src_ref=buf.at[pl.ds(0, count - 1)],
                dst_ref=buf.at[pl.ds(0, count - 1)],
                send_sem=send_sem.at[number],
                recv_sem=recv_sem.at[number],
                device_id=peer(1),
                device_id_type=MESH,
            )
            if sent:
                copy.wait_send()
            else:
                copy.wait_recv()

    plane_args = (planes, here, plane_peer, plane_send, plane_recv)
    line_args = (nx, gx, line_peer, line_send, line_recv)

    def plane_of(number):
        return plane_two if number else plane_one

    def line_of(number):
        return line_two if number else line_one

    def total_of(buf, count):
        total = buf[0]
        for i in range(1, count):
            total = total + buf[i]
        return total

    def reduce_middle(number):
        reduce_wait(number, plane_of(number), *plane_args, False)
        line_of(number)[gx] = total_of(plane_of(number), planes)
        reduce_start(number, line_of(number), *line_args)

    def reduce_end(number):
        reduce_wait(number, line_of(number), *line_args, False)
        return total_of(line_of(number), nx)

    def folded(x):
        return jnp.sum(x.reshape(x.shape[0] // 8, 8, lanes), axis=0)

    def add_sum(g, i, x):
        sums[g, i] = sums[g, i] + x

    local[0].wait()
    picks = [table[s % cap, s // cap] for s in range(slots)]
    index = [jnp.minimum(p, nblk - 1) for p in picks]
    mask = [jnp.minimum(nblk - p, 1).astype(F32) for p in picks]

    def gather_load(g, d):
        for k in range(cap):
            s = d * cap + k
            value = load_all[index[s], :, g * lanes : (g + 1) * lanes].astype(F32)
            if g:
                load_send[g - 1, d, k * blk : (k + 1) * blk] = value * mask[s]
            else:
                first_send[d, k * blk : (k + 1) * blk] = value * mask[s]

    def gather_prec(d):
        for k in range(cap):
            at = slice(rows + k * blk, rows + (k + 1) * blk)
            first_send[d, at] = prec_all[index[d * cap + k]]

    local[1].wait()
    for d in FAR:
        gather_load(0, d)
    local[2].wait()
    for d in FAR:
        gather_prec(d)
    gather_load(0, 0)
    gather_prec(0)
    pl.semaphore_wait(barrier, entered)
    for d in FAR:
        send("load", 0, d)
    gather_load(0, 1)
    gather_prec(1)
    send("load", 0, 0)
    gather_load(0, 4)
    gather_prec(4)
    send("load", 0, 1)
    gather_load(0, 5)
    gather_prec(5)
    send("load", 0, 4)
    for g in range(1, groups):
        for d in range(6):
            gather_load(g, d)
    send("load", 0, 5)
    sums[...] = jnp.zeros(sums.shape, F32)
    for d in range(6):
        @pl.when(jnp.logical_not(has[d]))
        def _(d=d):
            for g in range(groups):
                blank = jnp.zeros((cap, blk, lanes), F32)
                z1_ref[g, d * cap : (d + 1) * cap] = blank
                z2_ref[g, d * cap : (d + 1) * cap] = blank

    u1_send[...] = jnp.zeros(u1_send.shape, F32)
    u2_send[...] = jnp.zeros(u2_send.shape, F32)
    local[3].wait()
    eye = lax.broadcasted_iota(jnp.int32, (blk, blk), 0) == lax.broadcasted_iota(
        jnp.int32, (blk, blk), 1
    )
    for s in range(slots):
        column = jnp.sum(jnp.where(eye, diag_all[index[s]], 0.0), axis=1, keepdims=True)
        diag_slots[s * blk : (s + 1) * blk] = jnp.broadcast_to(column, (blk, lanes))
    relay("load", 0)
    for g in range(1, groups):
        for d in ORDER:
            send("load", g, d)
    pltpu.make_async_copy(schur_all, schur_all, local_sems.at[4]).wait()
    for s in range(slots):
        for t in range(slots):
            tile = schur_all[index[t], index[s]]
            schur_slots[s * blk : (s + 1) * blk, t * blk : (t + 1) * blk] = tile
    for g in range(1, groups):
        relay("load", g)

    def precondition(s, value):
        high = value.astype(BF16)
        low = (value - high.astype(F32)).astype(BF16)
        top = jnp.concatenate([high, low], axis=1)
        bottom = jnp.concatenate([high, jnp.zeros_like(low)], axis=1)
        z = jnp.dot(
            prec_split[s], jnp.concatenate([top, bottom], axis=0), preferred_element_type=F32
        )
        return z[:, :lanes] + z[:, lanes:]

    def narrowed(z):
        return jnp.concatenate([part.astype(BF16) for part in z], axis=0)

    def multiply(d, narrow, into, which):
        first, last = which[0], which[-1] + 1
        product = jnp.dot(
            schur_slots[first * rows : last * rows, d * rows : (d + 1) * rows],
            narrow,
            preferred_element_type=F32,
        )
        into[first:last] = into[first:last] + product.reshape(last - first, rows, lanes)

    def columns_of(z_ref, g, d):
        return narrowed([z_ref[g, d * cap + k] for k in range(cap)])

    def first_step(g, d):
        @pl.when(has[d])
        def _():
            arrived("load", g, d)
            if g == 0:
                for k in range(cap):
                    at = slice(rows + k * blk, rows + (k + 1) * blk)
                    block = first_send[d, at] + first_recv[d, at]
                    high = block.astype(BF16)
                    low = (block - high.astype(F32)).astype(BF16)
                    prec_split[d * cap + k] = jnp.concatenate([high, low], axis=1)
            z = []
            square = jnp.zeros((8, lanes), F32)
            for k in range(cap):
                at = slice(k * blk, (k + 1) * blk)
                if g:
                    value = load_send[g - 1, d, at] + load_recv[g - 1, d, at]
                else:
                    value = first_send[d, at] + first_recv[d, at]
                rhs[g, d, at] = value
                square = square + folded(value * value)
                z.append(precondition(d * cap + k, value))
                z1_ref[g, d * cap + k] = z[-1]
            add_sum(g, 0, square)
            multiply(d, narrowed(z), u1_send.at[g], ALL if d in NEAR else FAR)

    def second_step(g, d):
        @pl.when(has[d])
        def _():
            arrived("one", g, d)
            z = []
            for k in range(cap):
                s = d * cap + k
                at = slice(k * blk, (k + 1) * blk)
                value = (u1_send[g, d, at] + u1_recv[g, d, at]) * mask[s]
                a_ref[g, d, at] = value
                z.append(precondition(s, value))
                z2_ref[g, s] = z[-1]
            multiply(d, narrowed(z), u2_send.at[g], ALL if d in NEAR else FAR)

    def add_diagonal(z_ref, u_ref, g, d):
        scale = diag_slots[d * rows : (d + 1) * rows]
        u_ref[g, d] = u_ref[g, d] + scale * z_ref[g, d * cap : (d + 1) * cap].reshape(rows, lanes)

    def finish_far(g, z_ref, u_ref, kind):
        for d in FAR:
            @pl.when(has[d])
            def _(d=d):
                add_diagonal(z_ref, u_ref, g, d)

        for d in FAR:
            send(kind, g, d)

    def finish_near(g, z_ref, u_ref, kind):
        for d in FAR:
            @pl.when(has[d])
            def _(d=d):
                narrow = columns_of(z_ref, g, d)
                multiply(d, narrow, u_ref.at[g], (0, 1))
                multiply(d, narrow, u_ref.at[g], (4, 5))

        for d in (0, 1, 4, 5):
            @pl.when(has[d])
            def _(d=d):
                add_diagonal(z_ref, u_ref, g, d)

        for d in (0, 1, 4, 5):
            send(kind, g, d)

    def cross(g):
        for d in range(6):
            @pl.when(has[d])
            def _(d=d):
                add_sum(g, 1, folded(u1_send[g, d] * rhs[g, d]))

    def pack(values):
        return jnp.concatenate([jnp.sum(v, axis=0, keepdims=True) for v in values], axis=0)

    place = []
    for b in range(nblk):
        slot, live = jnp.int32(0), jnp.int32(0)
        for s in range(slots):
            same = 1 - jnp.minimum(jnp.abs(picks[s] - b), 1)
            slot, live = slot + s * same, live + same
        place.append((jnp.minimum(slot, slots - 1), live.astype(F32)))

    def spread(g, z_ref, z_out):
        for b in range(nblk):
            slot, live = place[b]
            z_out[b, :, g * lanes : (g + 1) * lanes] = z_ref[g, slot] * live

    last = groups - 1
    for g in range(groups):
        for d in NEAR:
            first_step(g, d)
        if g:
            relay("one", g - 1)
        for d in FAR:
            first_step(g, d)
        finish_far(g, z1_ref, u1_send, "one")
        finish_near(g, z1_ref, u1_send, "one")
        cross(g)
        spread(g, z1_ref, z1_out)

    for g in range(groups):
        if groups == 1:
            relay("one", last)
        for d in NEAR:
            second_step(g, d)
        if g == 0:
            packed = [pack((0.5 * sums[i, 0], sums[i, 1])) for i in range(groups)]
            plane_one[here] = jnp.concatenate(packed, axis=0)
            reduce_start(0, plane_one, *plane_args)
            if groups > 1:
                relay("one", last)
        else:
            relay("two", g - 1)
        for d in FAR:
            second_step(g, d)
        finish_far(g, z2_ref, u2_send, "two")
        if g == last:
            reduce_middle(0)
        finish_near(g, z2_ref, u2_send, "two")

    def measure(g, h11):
        for d in range(6):
            @pl.when(has[d])
            def _(d=d):
                square = jnp.zeros((8, lanes), F32)
                first = jnp.zeros((8, lanes), F32)
                second = jnp.zeros((8, lanes), F32)
                for k in range(cap):
                    at = slice(k * blk, (k + 1) * blk)
                    v = rhs[g, d, at]
                    q = a_ref[g, d, at] - h11 * v
                    u = u2_send[g, d, at] - h11 * u1_send[g, d, at]
                    square = square + folded(q * q)
                    first = first + folded(u * v)
                    second = second + folded(u * q)
                add_sum(g, 2, square)
                add_sum(g, 3, first)
                add_sum(g, 4, second)

    def third_step(g, d, h11):
        @pl.when(has[d])
        def _():
            arrived("two", g, d)
            begin = 0 if d % 2 == 0 else half
            work = jnp.zeros((8, lanes), F32)
            size = min(half, blk)
            for row in range(0, half, size):
                at = slice(begin + row, begin + row + size)
                w = (u2_send[g, d, at] + u2_recv[g, d, row : row + size]) * mask[d * cap + (begin + row) // blk]
                w = w - h11 * a_ref[g, d, at]
                work = work + folded(w * w)
            add_sum(g, 5, work)

    spread(0, z2_ref, z2_out)
    relay("two", last)
    total = reduce_end(0)
    squares = [total[2 * g : 2 * g + 1] for g in range(groups)]
    inners = [total[2 * g + 1 : 2 * g + 2] / (squares[g] + EPS) for g in range(groups)]
    measure(0, inners[0])
    for g in range(1, groups):
        spread(g, z2_ref, z2_out)
        measure(g, inners[g])
    for g in range(groups):
        for d in NEAR:
            third_step(g, d, inners[g])
        for d in FAR:
            third_step(g, d, inners[g])

    packed = []
    for g in range(groups):
        packed.append(pack((0.5 * sums[g, 2], sums[g, 3], sums[g, 4], sums[g, 5])))
    plane_two[here] = jnp.concatenate(packed, axis=0)
    reduce_start(1, plane_two, *plane_args)
    for g in range(groups):
        all_sent("two", g)
    reduce_wait(0, plane_one, *plane_args, True)
    reduce_wait(0, line_one, *line_args, True)
    reduce_middle(1)
    reduce_wait(1, plane_two, *plane_args, True)
    total = reduce_end(1)

    def both(rows_of):
        return jnp.concatenate(rows_of, axis=1)

    q_square, first, second, work = (
        both([total[4 * g + i : 4 * g + i + 1] for g in range(groups)]) for i in range(4)
    )
    load_square, h11 = both(squares), both(inners)
    beta = jnp.sqrt(load_square + EPS)
    inverse = 1.0 / beta
    h21 = jnp.sqrt(q_square * inverse * inverse + EPS)
    t = inverse / h21
    h12 = first * t * inverse
    a22 = second * t * t
    ww = work * t * t
    n1 = load_square * inverse * inverse
    n2 = q_square * t * t
    g12 = h11 * EPS * inverse * t
    h22 = a22 - h12 * g12
    left = (
        ww
        - h12 * h12 * (2.0 - n1)
        - h22 * (2.0 * a22 - h22 * n2)
        + 2.0 * h12 * h22 * g12
    )
    h32 = jnp.sqrt(jnp.maximum(left, 0.0) + EPS)
    r1 = jnp.sqrt(h11 * h11 + h21 * h21)
    c1 = h11 / r1
    s1 = h21 / r1
    top = c1 * h12 + s1 * h22
    low = c1 * h22 - s1 * h12
    r2 = jnp.sqrt(low * low + h32 * h32)
    c2 = low / r2
    s2 = h32 / r2
    y2 = -beta * s1 * c2 / r2
    y1 = (beta * c1 - top * y2) / r1
    weight2 = y2 * t
    final_ref[0:1] = y1 * inverse - weight2 * h11
    final_ref[1:2] = weight2
    final_ref[2:3] = beta * s1 * s2
    reduce_wait(1, line_two, *line_args, True)


def combine(z1, z2, final, out_ref, norm_ref, buf, norm_buf, sems):
    nblk = out_ref.shape[0]
    norm_buf[...] = final[2:3]
    copies = [pltpu.make_async_copy(norm_buf, norm_ref, sems.at[nblk])]
    copies[0].start()
    for b in range(nblk):
        buf[b] = final[0:1] * z1[b] + final[1:2] * z2[b]
        copies.append(pltpu.make_async_copy(buf.at[b], out_ref.at[b], sems.at[b]))
        copies[-1].start()
    for copy in copies:
        copy.wait()


def in_hbm(x):
    return pltpu.with_memory_space_constraint(x, pltpu.HBM)


def on_device(sizes, schur, interface_diag, precond, load, face_blocks):
    nblk, blk = precond.shape[3:5]
    cols = load.shape[-1]
    order = schur.shape[-1]
    cap = face_blocks.shape[-1]
    slots = 6 * cap
    rows = cap * blk
    nx, ny, nz = sizes
    planes = ny * nz
    groups = cols // LANES
    vmem = pltpu.VMEM
    dma = pltpu.SemaphoreType.DMA
    hbm = pl.BlockSpec(memory_space=pltpu.HBM)
    local = pl.BlockSpec(memory_space=pltpu.VMEM)
    scalars = pl.BlockSpec(memory_space=pltpu.SMEM)
    table = face_blocks.reshape(6, cap).T
    mib = 1024 * 1024
    z1, z2, final = pl.pallas_call(
        functools.partial(kernel, sizes),
        out_shape=(
            jax.ShapeDtypeStruct((nblk, blk, cols), F32),
            jax.ShapeDtypeStruct((nblk, blk, cols), F32),
            jax.ShapeDtypeStruct((3, cols), F32),
        ),
        in_specs=[hbm] * 5,
        out_specs=(local,) * 3,
        scratch_shapes=[
            pltpu.SMEM((cap, 6), jnp.int32),
            vmem((nblk, blk, cols), BF16),
            vmem((nblk, blk, blk), F32),
            vmem((nblk, 1, blk), F32),
            vmem((nblk, nblk, blk, blk), BF16),
            vmem((slots * blk, slots * blk), BF16),
            vmem((slots * blk, LANES), F32),
            vmem((6, 2 * rows, LANES), F32),
            vmem((6, 2 * rows, LANES), F32),
            vmem((max(groups - 1, 1), 6, rows, LANES), F32),
            vmem((max(groups - 1, 1), 6, rows, LANES), F32),
            vmem((slots, blk, 2 * blk), BF16),
            vmem((groups, 6, rows, LANES), F32),
            vmem((groups, 6, rows, LANES), F32),
            vmem((groups, slots, blk, LANES), F32),
            vmem((groups, slots, blk, LANES), F32),
            vmem((groups, 6, rows, LANES), F32),
            vmem((groups, 6, rows, LANES), F32),
            vmem((groups, 6, rows, LANES), F32),
            vmem((groups, 6, rows // 2, LANES), F32),
            vmem((rows, LANES), F32),
            vmem((2 * groups - 1, rows // 2, LANES), F32),
            vmem((max(groups - 1, 1), rows // 4, LANES), F32),
            vmem((rows // 8, LANES), F32),
            vmem((groups, 6, 8, LANES), F32),
            vmem((planes, 2 * groups, LANES), F32),
            vmem((nx, 2 * groups, LANES), F32),
            vmem((planes, 4 * groups, LANES), F32),
            vmem((nx, 4 * groups, LANES), F32),
            dma((5,)),
            dma((groups, 6)),
            dma((2 * groups, 6)),
            dma((groups,)),
            dma((2 * groups,)),
            dma((2,)),
            dma((2,)),
            dma((2,)),
            dma((2,)),
        ],
        compiler_params=pltpu.CompilerParams(
            collective_id=0, has_side_effects=True, vmem_limit_bytes=44 * mib
        ),
    )(
        in_hbm(table),
        in_hbm(schur.reshape(nblk, blk, order)),
        in_hbm(interface_diag.reshape(nblk, 1, blk)),
        in_hbm(precond.reshape(nblk, blk, blk)),
        in_hbm(load.reshape(nblk, blk, cols)),
    )
    result, norm = pl.pallas_call(
        combine,
        out_shape=(
            jax.ShapeDtypeStruct((nblk, blk, cols), F32),
            jax.ShapeDtypeStruct((1, cols), F32),
        ),
        in_specs=[local, local, local],
        out_specs=(hbm, hbm),
        scratch_shapes=[vmem((nblk, blk, cols), F32), vmem((1, cols), F32), dma((nblk + 1,))],
        compiler_params=pltpu.CompilerParams(vmem_limit_bytes=16 * mib),
    )(z1, z2, final)
    return result.reshape(1, 1, 1, nblk * blk, cols), norm.reshape(cols)


def solution(mesh):
    sizes = tuple(mesh.shape[a] for a in AXES)
    placed = (
        P("gx", "gy", "gz", None, None),
        P("gx", "gy", "gz", None),
        P("gx", "gy", "gz", None, None, None),
        P("gx", "gy", "gz", None, None),
        P("gx", "gy", "gz", None, None),
    )
    return jax.shard_map(
        functools.partial(on_device, sizes),
        mesh=mesh,
        in_specs=placed,
        out_specs=(P("gx", "gy", "gz", None, None), P()),
        check_vma=False,
    )
```

```python
import functools

import jax
import jax.numpy as jnp
from jax import lax
from jax.experimental import pallas as pl
from jax.experimental.pallas import tpu as pltpu
from jax.sharding import PartitionSpec as P

EPS = 1e-06
MESH = pl.DeviceIdType.MESH
AXES = ("gx", "gy", "gz")
LANES = 128
F32 = jnp.float32
BF16 = jnp.bfloat16
NEAR = (4, 5, 0, 1)
FAR = (2, 3)
ALL = (0, 1, 2, 3, 4, 5)


def kernel(
    sizes,
    table_hbm,
    schur_hbm,
    diag_hbm,
    prec_hbm,
    load_hbm,
    z1_out,
    z2_out,
    final_ref,
    table,
    load_all,
    prec_all,
    diag_all,
    schur_all,
    schur_slots,
    diag_slots,
    first_send,
    first_recv,
    load_send,
    load_recv,
    prec_split,
    rhs,
    a_ref,
    z1_ref,
    z2_ref,
    u1_send,
    u1_recv,
    u2_send,
    u2_recv,
    pass_first,
    pass_full,
    pass_half,
    sums,
    plane_one,
    line_one,
    plane_two,
    line_two,
    local_sems,
    face_send,
    face_recv,
    pass_send,
    pass_recv,
    plane_send,
    plane_recv,
    line_send,
    line_recv,
):
    nx, ny, nz = sizes
    planes = ny * nz
    groups, _, rows, lanes = rhs.shape
    nblk, blk = prec_hbm.shape[:2]
    cap = rows // blk
    slots = 6 * cap
    half = rows // 2
    gx, gy, gz = (lax.axis_index(a) for a in AXES)
    here = gy * nz + gz
    relayed = ny == 4 and nz == 2

    moves = [(table_hbm, table), (load_hbm, load_all), (prec_hbm, prec_all), (diag_hbm, diag_all)]
    local = [
        pltpu.make_async_copy(source, target, local_sems.at[i])
        for i, (source, target) in enumerate(moves)
    ]
    for copy in local:
        copy.start()

    def plane_peer(step):
        other = lax.rem(here + step, planes)
        return (gx, other // nz, lax.rem(other, nz))

    def line_peer(step):
        return (lax.rem(gx + step, nx), gy, gz)

    target, has = [], []
    for d in range(6):
        at = [gx, gy, gz]
        if d % 2 == 0:
            has.append(at[d // 2] + 1 < sizes[d // 2])
            at[d // 2] = at[d // 2] + 1
        else:
            has.append(at[d // 2] > 0)
            at[d // 2] = at[d // 2] - 1
        target.append(tuple(at))

    barrier = pltpu.get_barrier_semaphore()
    near = relayed and nx <= 4
    entered = jnp.int32(1)
    if near:
        for d in range(6):
            entered = entered + has[d].astype(jnp.int32)

            @pl.when(has[d])
            def _(d=d):
                pl.semaphore_signal(barrier, inc=1, device_id=target[d], device_id_type=MESH)

        pl.semaphore_signal(
            barrier, inc=1, device_id=(gx, lax.rem(gy + 2, ny), gz), device_id_type=MESH
        )
    else:
        entered = planes - 1 + nx - 1
        for step in range(1, planes):
            pl.semaphore_signal(barrier, inc=1, device_id=plane_peer(step), device_id_type=MESH)
        for step in range(1, nx):
            pl.semaphore_signal(barrier, inc=1, device_id=line_peer(step), device_id_type=MESH)

    def message(kind, g):
        if kind == "load" and g == 0:
            return g, g, first_send, first_recv, pass_first, 2 * rows, 0, rows
        if kind == "load":
            return g, g, load_send.at[g - 1], load_recv.at[g - 1], pass_full.at[g - 1], rows, 0, half
        if kind == "one":
            middle = pass_full.at[groups - 1 + g]
            return g, groups + g, u1_send.at[g], u1_recv.at[g], middle, rows, 0, half
        if g == groups - 1:
            return g, g, u2_send.at[g], u2_recv.at[g], None, half, half, 0
        return g, g, u2_send.at[g], u2_recv.at[g], pass_half.at[g], half, half, half // 2

    def before(kind, g):
        return {"load": None, "one": ("load", g), "two": ("one", g)}[kind]

    def ends(d):
        return (1, 3, 2) if d == 2 else (2, 0, 1)

    def face(msg, d, slot, device, row=0, size=None):
        g, number, source, landing, _, count, shift, _ = msg
        size = size or count
        begin = (shift if d % 2 == 0 else 0) + row
        return pltpu.make_async_remote_copy(
            src_ref=source.at[d, pl.ds(begin, size)],
            dst_ref=landing.at[slot, pl.ds(row, size)],
            send_sem=face_send.at[g, d],
            recv_sem=face_recv.at[number, slot],
            device_id=device,
            device_id_type=MESH,
        )

    def to_relay(msg, d):
        g, number, source, _, middle, count, shift, via = msg
        begin = (shift if d % 2 == 0 else 0) + count - via
        return pltpu.make_async_remote_copy(
            src_ref=source.at[d, pl.ds(begin, via)],
            dst_ref=middle,
            send_sem=face_send.at[g, d],
            recv_sem=pass_recv.at[number],
            device_id=(gx, ends(d)[1], gz),
            device_id_type=MESH,
        )

    def sent(msg, d):
        face(msg, d, d ^ 1, target[d]).wait_send()

    def send_far(kind, g, begin=0, end=None):
        msg = message(kind, g)
        count, via = msg[5], msg[7]
        end = end or count
        for d in FAR:
            @pl.when(has[d])
            def _(d=d):
                if before(kind, g):
                    sent(message(*before(kind, g)), d)

        if relayed:
            for d in FAR:
                @pl.when(gy == ends(d)[0])
                def _(d=d):
                    if via and end == count:
                        to_relay(msg, d).start()
                    if begin < count - via:
                        size = min(end, count - via) - begin
                        face(msg, d, d ^ 1, target[d], begin, size).start()

        for d in FAR:
            plain = jnp.logical_and(has[d], gy != ends(d)[0]) if relayed else has[d]

            @pl.when(plain)
            def _(d=d):
                face(msg, d, d ^ 1, target[d], begin, end - begin).start()

    def send(kind, g, d):
        msg = message(kind, g)

        @pl.when(has[d])
        def _():
            if before(kind, g):
                sent(message(*before(kind, g)), d)
            face(msg, d, d ^ 1, target[d]).start()

    def forward(msg, d):
        g, number, _, landing, middle, count, _, via = msg
        return pltpu.make_async_remote_copy(
            src_ref=middle,
            dst_ref=landing.at[d ^ 1, pl.ds(count - via, via)],
            send_sem=pass_send.at[g],
            recv_sem=face_recv.at[number, d ^ 1],
            device_id=(gx, ends(d)[2], gz),
            device_id_type=MESH,
        )

    def relay(kind, g):
        msg = message(kind, g)
        if not relayed or not msg[7]:
            return
        for d in FAR:
            @pl.when(gy == ends(d)[1])
            def _(d=d):
                to_relay(msg, d).wait_recv()
                if before(kind, g):
                    forward(message(*before(kind, g)), d).wait_send()
                forward(msg, d).start()

    def arrived(kind, g, d):
        face(message(kind, g), d, d, target[d]).wait_recv()

    def relay_sent(msg):
        if relayed and msg[7]:
            for d in FAR:
                @pl.when(gy == ends(d)[1])
                def _(d=d):
                    forward(msg, d).wait_send()

    def all_sent(kind, g):
        msg = message(kind, g)
        for d in range(6):
            @pl.when(has[d])
            def _(d=d):
                sent(msg, d)

        relay_sent(msg)

    def reduce_start(number, buf, count, me, peer, send_sem, recv_sem):
        for step in range(1, count):
            pltpu.make_async_remote_copy(
                src_ref=buf.at[me],
                dst_ref=buf.at[me],
                send_sem=send_sem.at[number],
                recv_sem=recv_sem.at[number],
                device_id=peer(step),
                device_id_type=MESH,
            ).start()

    def reduce_wait(number, buf, count, me, peer, send_sem, recv_sem, sent):
        if count > 1:
            copy = pltpu.make_async_remote_copy(
                src_ref=buf.at[pl.ds(0, count - 1)],
                dst_ref=buf.at[pl.ds(0, count - 1)],
                send_sem=send_sem.at[number],
                recv_sem=recv_sem.at[number],
                device_id=peer(1),
                device_id_type=MESH,
            )
            if sent:
                copy.wait_send()
            else:
                copy.wait_recv()

    plane_args = (planes, here, plane_peer, plane_send, plane_recv)
    line_args = (nx, gx, line_peer, line_send, line_recv)

    def plane_of(number):
        return plane_two if number else plane_one

    def line_of(number):
        return line_two if number else line_one

    def total_of(buf, count):
        total = buf[0]
        for i in range(1, count):
            total = total + buf[i]
        return total

    def reduce_middle(number):
        reduce_wait(number, plane_of(number), *plane_args, False)
        line_of(number)[gx] = total_of(plane_of(number), planes)
        reduce_start(number, line_of(number), *line_args)

    def reduce_end(number):
        reduce_wait(number, line_of(number), *line_args, False)
        return total_of(line_of(number), nx)

    def folded(x):
        return jnp.sum(x.reshape(x.shape[0] // 8, 8, lanes), axis=0)

    def add_sum(g, i, x):
        sums[g, i] = sums[g, i] + x

    local[0].wait()
    picks = [table[s % cap, s // cap] for s in range(slots)]
    index = [jnp.minimum(p, nblk - 1) for p in picks]
    mask = [jnp.minimum(nblk - p, 1).astype(F32) for p in picks]

    def gather_load(g, d):
        for k in range(cap):
            s = d * cap + k
            value = load_all[index[s], :, g * lanes : (g + 1) * lanes].astype(F32)
            if g:
                load_send[g - 1, d, k * blk : (k + 1) * blk] = value * mask[s]
            else:
                first_send[d, k * blk : (k + 1) * blk] = value * mask[s]

    def gather_prec(d):
        for k in range(cap):
            at = slice(rows + k * blk, rows + (k + 1) * blk)
            first_send[d, at] = prec_all[index[d * cap + k]]

    local[1].wait()
    for d in FAR:
        gather_load(0, d)
    pl.semaphore_wait(barrier, entered)
    send_far("load", 0, 0, rows)
    local[2].wait()
    for d in FAR:
        gather_prec(d)
    gather_load(0, 0)
    gather_prec(0)
    send_far("load", 0, rows, 2 * rows)
    gather_load(0, 1)
    gather_prec(1)
    send("load", 0, 0)
    gather_load(0, 4)
    gather_prec(4)
    send("load", 0, 1)
    gather_load(0, 5)
    gather_prec(5)
    send("load", 0, 4)
    for b in range(nblk):
        pltpu.make_async_copy(
            schur_hbm.at[:, :, pl.ds(b * blk, blk)], schur_all.at[b], local_sems.at[4]
        ).start()
    for g in range(1, groups):
        for d in range(6):
            gather_load(g, d)
    send("load", 0, 5)
    sums[...] = jnp.zeros(sums.shape, F32)
    for d in range(6):
        @pl.when(jnp.logical_not(has[d]))
        def _(d=d):
            for g in range(groups):
                blank = jnp.zeros((cap, blk, lanes), F32)
                z1_ref[g, d * cap : (d + 1) * cap] = blank
                z2_ref[g, d * cap : (d + 1) * cap] = blank

    u1_send[...] = jnp.zeros(u1_send.shape, F32)
    u2_send[...] = jnp.zeros(u2_send.shape, F32)
    local[3].wait()
    eye = lax.broadcasted_iota(jnp.int32, (blk, blk), 0) == lax.broadcasted_iota(
        jnp.int32, (blk, blk), 1
    )
    for s in range(slots):
        column = jnp.sum(jnp.where(eye, diag_all[index[s]], 0.0), axis=1, keepdims=True)
        diag_slots[s * blk : (s + 1) * blk] = jnp.broadcast_to(column, (blk, lanes))
    relay("load", 0)
    for g in range(1, groups):
        send_far("load", g)
        for d in (0, 1, 4, 5):
            send("load", g, d)
    pltpu.make_async_copy(schur_all, schur_all, local_sems.at[4]).wait()
    for s in range(slots):
        for t in range(slots):
            tile = schur_all[index[t], index[s]]
            schur_slots[s * blk : (s + 1) * blk, t * blk : (t + 1) * blk] = tile
    for g in range(1, groups):
        relay("load", g)

    def precondition(s, value):
        high = value.astype(BF16)
        low = (value - high.astype(F32)).astype(BF16)
        top = jnp.concatenate([high, low], axis=1)
        bottom = jnp.concatenate([high, jnp.zeros_like(low)], axis=1)
        z = jnp.dot(
            prec_split[s], jnp.concatenate([top, bottom], axis=0), preferred_element_type=F32
        )
        return z[:, :lanes] + z[:, lanes:]

    def narrowed(z):
        return jnp.concatenate([part.astype(BF16) for part in z], axis=0)

    def multiply(d, narrow, into, which):
        first, last = which[0], which[-1] + 1
        product = jnp.dot(
            schur_slots[first * rows : last * rows, d * rows : (d + 1) * rows],
            narrow,
            preferred_element_type=F32,
        )
        into[first:last] = into[first:last] + product.reshape(last - first, rows, lanes)

    def columns_of(z_ref, g, d):
        return narrowed([z_ref[g, d * cap + k] for k in range(cap)])

    def first_step(g, d):
        @pl.when(has[d])
        def _():
            arrived("load", g, d)
            if g == 0:
                for k in range(cap):
                    at = slice(rows + k * blk, rows + (k + 1) * blk)
                    block = first_send[d, at] + first_recv[d, at]
                    high = block.astype(BF16)
                    low = (block - high.astype(F32)).astype(BF16)
                    prec_split[d * cap + k] = jnp.concatenate([high, low], axis=1)
            z = []
            square = jnp.zeros((8, lanes), F32)
            for k in range(cap):
                at = slice(k * blk, (k + 1) * blk)
                if g:
                    value = load_send[g - 1, d, at] + load_recv[g - 1, d, at]
                else:
                    value = first_send[d, at] + first_recv[d, at]
                rhs[g, d, at] = value
                square = square + folded(value * value)
                z.append(precondition(d * cap + k, value))
                z1_ref[g, d * cap + k] = z[-1]
            add_sum(g, 0, square)
            multiply(d, narrowed(z), u1_send.at[g], ALL if d in NEAR else FAR)

    def second_step(g, d):
        @pl.when(has[d])
        def _():
            arrived("one", g, d)
            z = []
            for k in range(cap):
                s = d * cap + k
                at = slice(k * blk, (k + 1) * blk)
                value = (u1_send[g, d, at] + u1_recv[g, d, at]) * mask[s]
                a_ref[g, d, at] = value
                z.append(precondition(s, value))
                z2_ref[g, s] = z[-1]
            multiply(d, narrowed(z), u2_send.at[g], ALL if d in NEAR else FAR)

    def add_diagonal(z_ref, u_ref, g, d):
        scale = diag_slots[d * rows : (d + 1) * rows]
        u_ref[g, d] = u_ref[g, d] + scale * z_ref[g, d * cap : (d + 1) * cap].reshape(rows, lanes)

    def finish_far(g, z_ref, u_ref, kind):
        for d in FAR:
            @pl.when(has[d])
            def _(d=d):
                add_diagonal(z_ref, u_ref, g, d)

        send_far(kind, g)

    def finish_near(g, z_ref, u_ref, kind):
        for d in FAR:
            @pl.when(has[d])
            def _(d=d):
                narrow = columns_of(z_ref, g, d)
                multiply(d, narrow, u_ref.at[g], (0, 1))
                multiply(d, narrow, u_ref.at[g], (4, 5))

        for d in (0, 1, 4, 5):
            @pl.when(has[d])
            def _(d=d):
                add_diagonal(z_ref, u_ref, g, d)

        for d in (0, 1, 4, 5):
            send(kind, g, d)

    def cross(g):
        for d in range(6):
            @pl.when(has[d])
            def _(d=d):
                add_sum(g, 1, folded(u1_send[g, d] * rhs[g, d]))

    def pack(values):
        return jnp.concatenate([jnp.sum(v, axis=0, keepdims=True) for v in values], axis=0)

    place = []
    for b in range(nblk):
        slot, live = jnp.int32(0), jnp.int32(0)
        for s in range(slots):
            same = 1 - jnp.minimum(jnp.abs(picks[s] - b), 1)
            slot, live = slot + s * same, live + same
        place.append((jnp.minimum(slot, slots - 1), live.astype(F32)))

    def spread(g, z_ref, z_out):
        for b in range(nblk):
            slot, live = place[b]
            z_out[b, :, g * lanes : (g + 1) * lanes] = z_ref[g, slot] * live

    last = groups - 1
    for g in range(groups):
        for d in NEAR:
            first_step(g, d)
        if g:
            relay("one", g - 1)
        for d in FAR:
            first_step(g, d)
        finish_far(g, z1_ref, u1_send, "one")
        finish_near(g, z1_ref, u1_send, "one")
        cross(g)
        spread(g, z1_ref, z1_out)

    for g in range(groups):
        if groups == 1:
            relay("one", last)
        for d in NEAR:
            second_step(g, d)
        if g == 0:
            packed = [pack((0.5 * sums[i, 0], sums[i, 1])) for i in range(groups)]
            plane_one[here] = jnp.concatenate(packed, axis=0)
            reduce_start(0, plane_one, *plane_args)
            if groups > 1:
                relay("one", last)
        else:
            relay("two", g - 1)
        for d in FAR:
            second_step(g, d)
        finish_far(g, z2_ref, u2_send, "two")
        if g == last:
            reduce_middle(0)
        finish_near(g, z2_ref, u2_send, "two")

    def measure(g, h11):
        for d in range(6):
            @pl.when(has[d])
            def _(d=d):
                square = jnp.zeros((8, lanes), F32)
                first = jnp.zeros((8, lanes), F32)
                second = jnp.zeros((8, lanes), F32)
                for k in range(cap):
                    at = slice(k * blk, (k + 1) * blk)
                    v = rhs[g, d, at]
                    q = a_ref[g, d, at] - h11 * v
                    u = u2_send[g, d, at] - h11 * u1_send[g, d, at]
                    square = square + folded(q * q)
                    first = first + folded(u * v)
                    second = second + folded(u * q)
                add_sum(g, 2, square)
                add_sum(g, 3, first)
                add_sum(g, 4, second)

    def third_step(g, d, h11):
        @pl.when(has[d])
        def _():
            arrived("two", g, d)
            begin = 0 if d % 2 == 0 else half
            work = jnp.zeros((8, lanes), F32)
            size = min(half, blk)
            for row in range(0, half, size):
                at = slice(begin + row, begin + row + size)
                w = (u2_send[g, d, at] + u2_recv[g, d, row : row + size]) * mask[d * cap + (begin + row) // blk]
                w = w - h11 * a_ref[g, d, at]
                work = work + folded(w * w)
            add_sum(g, 5, work)

    spread(0, z2_ref, z2_out)
    relay("two", last)
    total = reduce_end(0)
    squares = [total[2 * g : 2 * g + 1] for g in range(groups)]
    inners = [total[2 * g + 1 : 2 * g + 2] / (squares[g] + EPS) for g in range(groups)]
    measure(0, inners[0])
    for g in range(1, groups):
        spread(g, z2_ref, z2_out)
        measure(g, inners[g])
    for g in range(groups):
        for d in NEAR:
            third_step(g, d, inners[g])
        for d in FAR:
            third_step(g, d, inners[g])

    packed = []
    for g in range(groups):
        packed.append(pack((0.5 * sums[g, 2], sums[g, 3], sums[g, 4], sums[g, 5])))
    plane_two[here] = jnp.concatenate(packed, axis=0)
    reduce_start(1, plane_two, *plane_args)
    for g in range(groups):
        all_sent("two", g)
    relay_sent(message("one", last))
    reduce_wait(0, plane_one, *plane_args, True)
    reduce_wait(0, line_one, *line_args, True)
    reduce_middle(1)
    reduce_wait(1, plane_two, *plane_args, True)
    total = reduce_end(1)

    def both(rows_of):
        return jnp.concatenate(rows_of, axis=1)

    q_square, first, second, work = (
        both([total[4 * g + i : 4 * g + i + 1] for g in range(groups)]) for i in range(4)
    )
    load_square, h11 = both(squares), both(inners)
    beta = jnp.sqrt(load_square + EPS)
    inverse = 1.0 / beta
    h21 = jnp.sqrt(q_square * inverse * inverse + EPS)
    t = inverse / h21
    h12 = first * t * inverse
    a22 = second * t * t
    ww = work * t * t
    n1 = load_square * inverse * inverse
    n2 = q_square * t * t
    g12 = h11 * EPS * inverse * t
    h22 = a22 - h12 * g12
    left = (
        ww
        - h12 * h12 * (2.0 - n1)
        - h22 * (2.0 * a22 - h22 * n2)
        + 2.0 * h12 * h22 * g12
    )
    h32 = jnp.sqrt(jnp.maximum(left, 0.0) + EPS)
    r1 = jnp.sqrt(h11 * h11 + h21 * h21)
    c1 = h11 / r1
    s1 = h21 / r1
    top = c1 * h12 + s1 * h22
    low = c1 * h22 - s1 * h12
    r2 = jnp.sqrt(low * low + h32 * h32)
    c2 = low / r2
    s2 = h32 / r2
    y2 = -beta * s1 * c2 / r2
    y1 = (beta * c1 - top * y2) / r1
    weight2 = y2 * t
    final_ref[0:1] = y1 * inverse - weight2 * h11
    final_ref[1:2] = weight2
    final_ref[2:3] = beta * s1 * s2
    reduce_wait(1, line_two, *line_args, True)


def combine(z1, z2, final, out_ref, norm_ref, buf, norm_buf, sems):
    nblk = out_ref.shape[0]
    norm_buf[...] = final[2:3]
    norm_copy = pltpu.make_async_copy(norm_buf, norm_ref, sems.at[1])
    norm_copy.start()
    for b in range(nblk):
        buf[b] = final[0:1] * z1[b] + final[1:2] * z2[b]
        pltpu.make_async_copy(buf.at[b], out_ref.at[b], sems.at[0]).start()
    pltpu.make_async_copy(buf, out_ref, sems.at[0]).wait()
    norm_copy.wait()


def in_hbm(x):
    return pltpu.with_memory_space_constraint(x, pltpu.HBM)


def on_device(sizes, schur, interface_diag, precond, load, face_blocks):
    nblk, blk = precond.shape[3:5]
    cols = load.shape[-1]
    order = schur.shape[-1]
    cap = face_blocks.shape[-1]
    slots = 6 * cap
    rows = cap * blk
    nx, ny, nz = sizes
    planes = ny * nz
    groups = cols // LANES
    vmem = pltpu.VMEM
    dma = pltpu.SemaphoreType.DMA
    hbm = pl.BlockSpec(memory_space=pltpu.HBM)
    local = pl.BlockSpec(memory_space=pltpu.VMEM)
    scalars = pl.BlockSpec(memory_space=pltpu.SMEM)
    table = face_blocks.reshape(6, cap).T
    mib = 1024 * 1024
    z1, z2, final = pl.pallas_call(
        functools.partial(kernel, sizes),
        out_shape=(
            jax.ShapeDtypeStruct((nblk, blk, cols), F32),
            jax.ShapeDtypeStruct((nblk, blk, cols), F32),
            jax.ShapeDtypeStruct((3, cols), F32),
        ),
        in_specs=[hbm] * 5,
        out_specs=(local,) * 3,
        scratch_shapes=[
            pltpu.SMEM((cap, 6), jnp.int32),
            vmem((nblk, blk, cols), BF16),
            vmem((nblk, blk, blk), F32),
            vmem((nblk, 1, blk), F32),
            vmem((nblk, nblk, blk, blk), BF16),
            vmem((slots * blk, slots * blk), BF16),
            vmem((slots * blk, LANES), F32),
            vmem((6, 2 * rows, LANES), F32),
            vmem((6, 2 * rows, LANES), F32),
            vmem((max(groups - 1, 1), 6, rows, LANES), F32),
            vmem((max(groups - 1, 1), 6, rows, LANES), F32),
            vmem((slots, blk, 2 * blk), BF16),
            vmem((groups, 6, rows, LANES), F32),
            vmem((groups, 6, rows, LANES), F32),
            vmem((groups, slots, blk, LANES), F32),
            vmem((groups, slots, blk, LANES), F32),
            vmem((groups, 6, rows, LANES), F32),
            vmem((groups, 6, rows, LANES), F32),
            vmem((groups, 6, rows, LANES), F32),
            vmem((groups, 6, rows // 2, LANES), F32),
            vmem((rows, LANES), F32),
            vmem((2 * groups - 1, rows // 2, LANES), F32),
            vmem((max(groups - 1, 1), rows // 4, LANES), F32),
            vmem((groups, 6, 8, LANES), F32),
            vmem((planes, 2 * groups, LANES), F32),
            vmem((nx, 2 * groups, LANES), F32),
            vmem((planes, 4 * groups, LANES), F32),
            vmem((nx, 4 * groups, LANES), F32),
            dma((5,)),
            dma((groups, 6)),
            dma((2 * groups, 6)),
            dma((groups,)),
            dma((2 * groups,)),
            dma((2,)),
            dma((2,)),
            dma((2,)),
            dma((2,)),
        ],
        compiler_params=pltpu.CompilerParams(
            collective_id=0, has_side_effects=True, vmem_limit_bytes=44 * mib
        ),
    )(
        in_hbm(table),
        in_hbm(schur.reshape(nblk, blk, order)),
        in_hbm(interface_diag.reshape(nblk, 1, blk)),
        in_hbm(precond.reshape(nblk, blk, blk)),
        in_hbm(load.reshape(nblk, blk, cols)),
    )
    result, norm = pl.pallas_call(
        combine,
        out_shape=(
            jax.ShapeDtypeStruct((nblk, blk, cols), F32),
            jax.ShapeDtypeStruct((1, cols), F32),
        ),
        in_specs=[local, local, local],
        out_specs=(hbm, hbm),
        scratch_shapes=[vmem((nblk, blk, cols), F32), vmem((1, cols), F32), dma((2,))],
        compiler_params=pltpu.CompilerParams(vmem_limit_bytes=16 * mib),
    )(z1, z2, final)
    return result.reshape(1, 1, 1, nblk * blk, cols), norm.reshape(cols)


def solution(mesh):
    sizes = tuple(mesh.shape[a] for a in AXES)
    placed = (
        P("gx", "gy", "gz", None, None),
        P("gx", "gy", "gz", None),
        P("gx", "gy", "gz", None, None, None),
        P("gx", "gy", "gz", None, None),
        P("gx", "gy", "gz", None, None),
    )
    return jax.shard_map(
        functools.partial(on_device, sizes),
        mesh=mesh,
        in_specs=placed,
        out_specs=(P("gx", "gy", "gz", None, None), P()),
        check_vma=False,
    )
```

```python
import functools

import jax
import jax.numpy as jnp
from jax import lax
from jax.experimental import pallas as pl
from jax.experimental.pallas import tpu as pltpu
from jax.sharding import PartitionSpec as P

EPS = 1e-06
MESH = pl.DeviceIdType.MESH
AXES = ("gx", "gy", "gz")
LANES = 128
F32 = jnp.float32
BF16 = jnp.bfloat16
NEAR = (4, 5, 0, 1)
FAR = (2, 3)
ALL = (0, 1, 2, 3, 4, 5)


def kernel(
    sizes,
    table_hbm,
    schur_hbm,
    diag_hbm,
    prec_hbm,
    load_hbm,
    z1_out,
    z2_out,
    final_ref,
    table,
    load_all,
    prec_all,
    diag_all,
    schur_all,
    schur_slots,
    diag_slots,
    first_send,
    first_recv,
    load_send,
    load_recv,
    prec_split,
    rhs,
    a_ref,
    z1_ref,
    z2_ref,
    u1_send,
    u1_recv,
    u2_send,
    u2_recv,
    pass_first,
    pass_full,
    pass_half,
    sums,
    plane_one,
    line_one,
    plane_two,
    line_two,
    local_sems,
    face_send,
    face_recv,
    pass_send,
    pass_recv,
    plane_send,
    plane_recv,
    line_send,
    line_recv,
):
    nx, ny, nz = sizes
    planes = ny * nz
    groups, _, rows, lanes = rhs.shape
    nblk, blk = prec_hbm.shape[:2]
    cap = rows // blk
    slots = 6 * cap
    half = rows // 2
    gx, gy, gz = (lax.axis_index(a) for a in AXES)
    here = gy * nz + gz
    relayed = ny == 4 and nz == 2

    moves = [(table_hbm, table), (load_hbm, load_all), (prec_hbm, prec_all), (diag_hbm, diag_all)]
    local = [
        pltpu.make_async_copy(source, target, local_sems.at[i])
        for i, (source, target) in enumerate(moves)
    ]
    for copy in local:
        copy.start()

    def plane_peer(step):
        other = lax.rem(here + step, planes)
        return (gx, other // nz, lax.rem(other, nz))

    def line_peer(step):
        return (lax.rem(gx + step, nx), gy, gz)

    target, has = [], []
    for d in range(6):
        at = [gx, gy, gz]
        if d % 2 == 0:
            has.append(at[d // 2] + 1 < sizes[d // 2])
            at[d // 2] = at[d // 2] + 1
        else:
            has.append(at[d // 2] > 0)
            at[d // 2] = at[d // 2] - 1
        target.append(tuple(at))

    barrier = pltpu.get_barrier_semaphore()
    near = relayed and nx <= 4
    entered = jnp.int32(1)
    if near:
        for d in range(6):
            entered = entered + has[d].astype(jnp.int32)

            @pl.when(has[d])
            def _(d=d):
                pl.semaphore_signal(barrier, inc=1, device_id=target[d], device_id_type=MESH)

        pl.semaphore_signal(
            barrier, inc=1, device_id=(gx, lax.rem(gy + 2, ny), gz), device_id_type=MESH
        )
    else:
        entered = planes - 1 + nx - 1
        for step in range(1, planes):
            pl.semaphore_signal(barrier, inc=1, device_id=plane_peer(step), device_id_type=MESH)
        for step in range(1, nx):
            pl.semaphore_signal(barrier, inc=1, device_id=line_peer(step), device_id_type=MESH)

    def message(kind, g):
        if kind == "load" and g == 0:
            return g, g, first_send, first_recv, pass_first, 2 * rows, 0, rows
        if kind == "load":
            return g, g, load_send.at[g - 1], load_recv.at[g - 1], pass_full.at[g - 1], rows, 0, half
        if kind == "one":
            middle = pass_full.at[groups - 1 + g]
            return g, groups + g, u1_send.at[g], u1_recv.at[g], middle, rows, 0, half
        if g == groups - 1:
            return g, g, u2_send.at[g], u2_recv.at[g], None, half, half, 0
        return g, g, u2_send.at[g], u2_recv.at[g], pass_half.at[g], half, half, half // 2

    def before(kind, g):
        return {"load": None, "one": ("load", g), "two": ("one", g)}[kind]

    def ends(d):
        return (1, 3, 2) if d == 2 else (2, 0, 1)

    def face(msg, d, slot, device, row=0, size=None):
        g, number, source, landing, _, count, shift, _ = msg
        size = size or count
        begin = (shift if d % 2 == 0 else 0) + row
        return pltpu.make_async_remote_copy(
            src_ref=source.at[d, pl.ds(begin, size)],
            dst_ref=landing.at[slot, pl.ds(row, size)],
            send_sem=face_send.at[g, d],
            recv_sem=face_recv.at[number, slot],
            device_id=device,
            device_id_type=MESH,
        )

    def to_relay(msg, d):
        g, number, source, _, middle, count, shift, via = msg
        begin = (shift if d % 2 == 0 else 0) + count - via
        return pltpu.make_async_remote_copy(
            src_ref=source.at[d, pl.ds(begin, via)],
            dst_ref=middle,
            send_sem=face_send.at[g, d],
            recv_sem=pass_recv.at[number],
            device_id=(gx, ends(d)[1], gz),
            device_id_type=MESH,
        )

    def sent(msg, d):
        face(msg, d, d ^ 1, target[d]).wait_send()

    def send_far(kind, g, begin=0, end=None):
        msg = message(kind, g)
        count, via = msg[5], msg[7]
        end = end or count
        for d in FAR:
            @pl.when(has[d])
            def _(d=d):
                if before(kind, g):
                    sent(message(*before(kind, g)), d)

        if relayed:
            for d in FAR:
                @pl.when(gy == ends(d)[0])
                def _(d=d):
                    if via and end == count:
                        to_relay(msg, d).start()
                    if begin < count - via:
                        size = min(end, count - via) - begin
                        face(msg, d, d ^ 1, target[d], begin, size).start()

        for d in FAR:
            plain = jnp.logical_and(has[d], gy != ends(d)[0]) if relayed else has[d]

            @pl.when(plain)
            def _(d=d):
                face(msg, d, d ^ 1, target[d], begin, end - begin).start()

    def send(kind, g, d):
        msg = message(kind, g)

        @pl.when(has[d])
        def _():
            if before(kind, g):
                sent(message(*before(kind, g)), d)
            face(msg, d, d ^ 1, target[d]).start()

    def forward(msg, d):
        g, number, _, landing, middle, count, _, via = msg
        return pltpu.make_async_remote_copy(
            src_ref=middle,
            dst_ref=landing.at[d ^ 1, pl.ds(count - via, via)],
            send_sem=pass_send.at[g],
            recv_sem=face_recv.at[number, d ^ 1],
            device_id=(gx, ends(d)[2], gz),
            device_id_type=MESH,
        )

    def relay(kind, g):
        msg = message(kind, g)
        if not relayed or not msg[7]:
            return
        for d in FAR:
            @pl.when(gy == ends(d)[1])
            def _(d=d):
                to_relay(msg, d).wait_recv()
                if before(kind, g):
                    forward(message(*before(kind, g)), d).wait_send()
                forward(msg, d).start()

    def arrived(kind, g, d):
        face(message(kind, g), d, d, target[d]).wait_recv()

    def relay_sent(msg):
        if relayed and msg[7]:
            for d in FAR:
                @pl.when(gy == ends(d)[1])
                def _(d=d):
                    forward(msg, d).wait_send()

    def all_sent(kind, g):
        msg = message(kind, g)
        for d in range(6):
            @pl.when(has[d])
            def _(d=d):
                sent(msg, d)

        relay_sent(msg)

    def plane_of(number):
        return plane_two if number else plane_one

    def line_of(number):
        return line_two if number else line_one

    def part_copy(number, buf, slot, device, send_sem, recv_sem):
        return pltpu.make_async_remote_copy(
            src_ref=buf.at[slot],
            dst_ref=buf.at[slot],
            send_sem=send_sem.at[number],
            recv_sem=recv_sem.at[number],
            device_id=device,
            device_id_type=MESH,
        )

    def parts_wait(number, count, send_sem, recv_sem, sent):
        if count:
            buf = plane_of(number)
            copy = part_copy(
                number, buf, pl.ds(0, count), line_peer(1), send_sem, recv_sem
            )
            if sent:
                copy.wait_send()
            else:
                copy.wait_recv()

    hub = nz - 1
    is_hub = gz == hub

    def reduce_start(number):
        buf = plane_of(number)
        if not relayed:
            for step in range(1, planes):
                part_copy(number, buf, here, plane_peer(step), plane_send, plane_recv).start()
            return
        for step in range(1, ny):
            device = (gx, lax.rem(gy + step, ny), hub)
            part_copy(number, buf, here, device, plane_send, plane_recv).start()

        @pl.when(jnp.logical_not(is_hub))
        def _():
            part_copy(number, buf, here, (gx, gy, hub), plane_send, plane_recv).start()

    def reduce_middle(number):
        line = line_of(number)
        if not relayed:
            parts_wait(number, planes - 1, plane_send, plane_recv, False)
            line[gx] = total_of(plane_of(number), planes)
            for step in range(1, nx):
                part_copy(number, line, gx, line_peer(step), line_send, line_recv).start()
            return

        @pl.when(is_hub)
        def _():
            parts_wait(number, planes - 1, plane_send, plane_recv, False)
            line[gx] = total_of(plane_of(number), planes)
            for core in range(nz):
                for step in range(1, nx):
                    device = (lax.rem(gx + nx - step, nx), gy, core)
                    part_copy(number, line, gx, device, line_send, line_recv).start()
            part_copy(number, line, gx, (gx, gy, 0), line_send, line_recv).start()

    def reduce_end(number):
        if relayed:
            for core in range(nz):
                @pl.when(gz == core)
                def _(core=core):
                    parts_wait(number, nx - (core == hub), line_send, line_recv, False)
        else:
            parts_wait(number, nx - 1, line_send, line_recv, False)
        return total_of(line_of(number), nx)

    def reduce_sent(number):
        if not relayed:
            parts_wait(number, planes - 1, plane_send, plane_recv, True)
            parts_wait(number, nx - 1, line_send, line_recv, True)
            return
        for core in range(nz):
            @pl.when(gz == core)
            def _(core=core):
                parts_wait(number, ny - (core == hub), plane_send, plane_recv, True)
                if core == hub:
                    parts_wait(number, nz * (nx - 1) + 1, line_send, line_recv, True)

    def total_of(buf, count):
        total = buf[0]
        for i in range(1, count):
            total = total + buf[i]
        return total

    def folded(x):
        return jnp.sum(x.reshape(x.shape[0] // 8, 8, lanes), axis=0)

    def add_sum(g, i, x):
        sums[g, i] = sums[g, i] + x

    local[0].wait()
    picks = [table[s % cap, s // cap] for s in range(slots)]
    index = [jnp.minimum(p, nblk - 1) for p in picks]
    mask = [jnp.minimum(nblk - p, 1).astype(F32) for p in picks]

    def gather_load(g, d):
        for k in range(cap):
            s = d * cap + k
            value = load_all[index[s], :, g * lanes : (g + 1) * lanes].astype(F32)
            if g:
                load_send[g - 1, d, k * blk : (k + 1) * blk] = value * mask[s]
            else:
                first_send[d, k * blk : (k + 1) * blk] = value * mask[s]

    def gather_prec(d):
        for k in range(cap):
            at = slice(rows + k * blk, rows + (k + 1) * blk)
            first_send[d, at] = prec_all[index[d * cap + k]]

    local[1].wait()
    for d in FAR:
        gather_load(0, d)
    pl.semaphore_wait(barrier, entered)
    send_far("load", 0, 0, rows)
    local[2].wait()
    for d in FAR:
        gather_prec(d)
    gather_load(0, 0)
    gather_prec(0)
    send_far("load", 0, rows, 2 * rows)
    gather_load(0, 1)
    gather_prec(1)
    send("load", 0, 0)
    gather_load(0, 4)
    gather_prec(4)
    send("load", 0, 1)
    gather_load(0, 5)
    gather_prec(5)
    send("load", 0, 4)
    for b in range(nblk):
        pltpu.make_async_copy(
            schur_hbm.at[:, :, pl.ds(b * blk, blk)], schur_all.at[b], local_sems.at[4]
        ).start()
    for g in range(1, groups):
        for d in range(6):
            gather_load(g, d)
    send("load", 0, 5)
    sums[...] = jnp.zeros(sums.shape, F32)
    for d in range(6):
        @pl.when(jnp.logical_not(has[d]))
        def _(d=d):
            for g in range(groups):
                blank = jnp.zeros((cap, blk, lanes), F32)
                z1_ref[g, d * cap : (d + 1) * cap] = blank
                z2_ref[g, d * cap : (d + 1) * cap] = blank

    u1_send[...] = jnp.zeros(u1_send.shape, F32)
    u2_send[...] = jnp.zeros(u2_send.shape, F32)
    local[3].wait()
    eye = lax.broadcasted_iota(jnp.int32, (blk, blk), 0) == lax.broadcasted_iota(
        jnp.int32, (blk, blk), 1
    )
    for s in range(slots):
        column = jnp.sum(jnp.where(eye, diag_all[index[s]], 0.0), axis=1, keepdims=True)
        diag_slots[s * blk : (s + 1) * blk] = jnp.broadcast_to(column, (blk, lanes))
    relay("load", 0)
    for g in range(1, groups):
        send_far("load", g)
        for d in (0, 1, 4, 5):
            send("load", g, d)
    pltpu.make_async_copy(schur_all, schur_all, local_sems.at[4]).wait()
    for s in range(slots):
        for t in range(slots):
            tile = schur_all[index[t], index[s]]
            schur_slots[s * blk : (s + 1) * blk, t * blk : (t + 1) * blk] = tile
    for g in range(1, groups):
        relay("load", g)

    def precondition(s, value):
        high = value.astype(BF16)
        low = (value - high.astype(F32)).astype(BF16)
        top = jnp.concatenate([high, low], axis=1)
        bottom = jnp.concatenate([high, jnp.zeros_like(low)], axis=1)
        z = jnp.dot(
            prec_split[s], jnp.concatenate([top, bottom], axis=0), preferred_element_type=F32
        )
        return z[:, :lanes] + z[:, lanes:]

    def narrowed(z):
        return jnp.concatenate([part.astype(BF16) for part in z], axis=0)

    def multiply(d, narrow, into, which):
        first, last = which[0], which[-1] + 1
        product = jnp.dot(
            schur_slots[first * rows : last * rows, d * rows : (d + 1) * rows],
            narrow,
            preferred_element_type=F32,
        )
        into[first:last] = into[first:last] + product.reshape(last - first, rows, lanes)

    def columns_of(z_ref, g, d):
        return narrowed([z_ref[g, d * cap + k] for k in range(cap)])

    def first_step(g, d):
        @pl.when(has[d])
        def _():
            arrived("load", g, d)
            if g == 0:
                for k in range(cap):
                    at = slice(rows + k * blk, rows + (k + 1) * blk)
                    block = first_send[d, at] + first_recv[d, at]
                    high = block.astype(BF16)
                    low = (block - high.astype(F32)).astype(BF16)
                    prec_split[d * cap + k] = jnp.concatenate([high, low], axis=1)
            z = []
            square = jnp.zeros((8, lanes), F32)
            for k in range(cap):
                at = slice(k * blk, (k + 1) * blk)
                if g:
                    value = load_send[g - 1, d, at] + load_recv[g - 1, d, at]
                else:
                    value = first_send[d, at] + first_recv[d, at]
                rhs[g, d, at] = value
                square = square + folded(value * value)
                z.append(precondition(d * cap + k, value))
                z1_ref[g, d * cap + k] = z[-1]
            add_sum(g, 0, square)
            multiply(d, narrowed(z), u1_send.at[g], ALL if d in NEAR else FAR)

    def second_step(g, d):
        @pl.when(has[d])
        def _():
            arrived("one", g, d)
            z = []
            for k in range(cap):
                s = d * cap + k
                at = slice(k * blk, (k + 1) * blk)
                value = (u1_send[g, d, at] + u1_recv[g, d, at]) * mask[s]
                a_ref[g, d, at] = value
                z.append(precondition(s, value))
                z2_ref[g, s] = z[-1]
            multiply(d, narrowed(z), u2_send.at[g], ALL if d in NEAR else FAR)

    def add_diagonal(z_ref, u_ref, g, d):
        scale = diag_slots[d * rows : (d + 1) * rows]
        u_ref[g, d] = u_ref[g, d] + scale * z_ref[g, d * cap : (d + 1) * cap].reshape(rows, lanes)

    def finish_far(g, z_ref, u_ref, kind):
        for d in FAR:
            @pl.when(has[d])
            def _(d=d):
                add_diagonal(z_ref, u_ref, g, d)

        send_far(kind, g)

    def finish_near(g, z_ref, u_ref, kind):
        for d in FAR:
            @pl.when(has[d])
            def _(d=d):
                narrow = columns_of(z_ref, g, d)
                multiply(d, narrow, u_ref.at[g], (0, 1))
                multiply(d, narrow, u_ref.at[g], (4, 5))

        for d in (0, 1, 4, 5):
            @pl.when(has[d])
            def _(d=d):
                add_diagonal(z_ref, u_ref, g, d)

        for d in (0, 1, 4, 5):
            send(kind, g, d)

    def cross(g):
        for d in range(6):
            @pl.when(has[d])
            def _(d=d):
                add_sum(g, 1, folded(u1_send[g, d] * rhs[g, d]))

    def pack(values):
        return jnp.concatenate([jnp.sum(v, axis=0, keepdims=True) for v in values], axis=0)

    place = []
    for b in range(nblk):
        slot, live = jnp.int32(0), jnp.int32(0)
        for s in range(slots):
            same = 1 - jnp.minimum(jnp.abs(picks[s] - b), 1)
            slot, live = slot + s * same, live + same
        place.append((jnp.minimum(slot, slots - 1), live.astype(F32)))

    def spread(g, z_ref, z_out):
        for b in range(nblk):
            slot, live = place[b]
            z_out[b, :, g * lanes : (g + 1) * lanes] = z_ref[g, slot] * live

    last = groups - 1
    for g in range(groups):
        for d in NEAR:
            first_step(g, d)
        if g:
            relay("one", g - 1)
        for d in FAR:
            first_step(g, d)
        finish_far(g, z1_ref, u1_send, "one")
        finish_near(g, z1_ref, u1_send, "one")
        cross(g)
        spread(g, z1_ref, z1_out)

    for g in range(groups):
        if groups == 1:
            relay("one", last)
        for d in NEAR:
            second_step(g, d)
        if g == 0:
            packed = [pack((0.5 * sums[i, 0], sums[i, 1])) for i in range(groups)]
            plane_one[here] = jnp.concatenate(packed, axis=0)
            reduce_start(0)
            if groups > 1:
                relay("one", last)
        else:
            relay("two", g - 1)
        for d in FAR:
            second_step(g, d)
        finish_far(g, z2_ref, u2_send, "two")
        if g == last:
            reduce_middle(0)
        finish_near(g, z2_ref, u2_send, "two")

    def measure(g, h11):
        for d in range(6):
            @pl.when(has[d])
            def _(d=d):
                square = jnp.zeros((8, lanes), F32)
                first = jnp.zeros((8, lanes), F32)
                second = jnp.zeros((8, lanes), F32)
                for k in range(cap):
                    at = slice(k * blk, (k + 1) * blk)
                    v = rhs[g, d, at]
                    q = a_ref[g, d, at] - h11 * v
                    u = u2_send[g, d, at] - h11 * u1_send[g, d, at]
                    square = square + folded(q * q)
                    first = first + folded(u * v)
                    second = second + folded(u * q)
                add_sum(g, 2, square)
                add_sum(g, 3, first)
                add_sum(g, 4, second)

    def third_step(g, d, h11):
        @pl.when(has[d])
        def _():
            arrived("two", g, d)
            begin = 0 if d % 2 == 0 else half
            work = jnp.zeros((8, lanes), F32)
            size = min(half, blk)
            for row in range(0, half, size):
                at = slice(begin + row, begin + row + size)
                w = (u2_send[g, d, at] + u2_recv[g, d, row : row + size]) * mask[d * cap + (begin + row) // blk]
                w = w - h11 * a_ref[g, d, at]
                work = work + folded(w * w)
            add_sum(g, 5, work)

    spread(0, z2_ref, z2_out)
    relay("two", last)
    total = reduce_end(0)
    squares = [total[2 * g : 2 * g + 1] for g in range(groups)]
    inners = [total[2 * g + 1 : 2 * g + 2] / (squares[g] + EPS) for g in range(groups)]
    measure(0, inners[0])
    for g in range(1, groups):
        spread(g, z2_ref, z2_out)
        measure(g, inners[g])
    for g in range(groups):
        for d in NEAR:
            third_step(g, d, inners[g])
        for d in FAR:
            third_step(g, d, inners[g])

    packed = []
    for g in range(groups):
        packed.append(pack((0.5 * sums[g, 2], sums[g, 3], sums[g, 4], sums[g, 5])))
    plane_two[here] = jnp.concatenate(packed, axis=0)
    reduce_start(1)
    for g in range(groups):
        all_sent("two", g)
    relay_sent(message("one", last))
    reduce_sent(0)
    reduce_middle(1)
    total = reduce_end(1)

    def both(rows_of):
        return jnp.concatenate(rows_of, axis=1)

    q_square, first, second, work = (
        both([total[4 * g + i : 4 * g + i + 1] for g in range(groups)]) for i in range(4)
    )
    load_square, h11 = both(squares), both(inners)
    beta = jnp.sqrt(load_square + EPS)
    inverse = 1.0 / beta
    h21 = jnp.sqrt(q_square * inverse * inverse + EPS)
    t = inverse / h21
    h12 = first * t * inverse
    a22 = second * t * t
    ww = work * t * t
    n1 = load_square * inverse * inverse
    n2 = q_square * t * t
    g12 = h11 * EPS * inverse * t
    h22 = a22 - h12 * g12
    left = (
        ww
        - h12 * h12 * (2.0 - n1)
        - h22 * (2.0 * a22 - h22 * n2)
        + 2.0 * h12 * h22 * g12
    )
    h32 = jnp.sqrt(jnp.maximum(left, 0.0) + EPS)
    r1 = jnp.sqrt(h11 * h11 + h21 * h21)
    c1 = h11 / r1
    s1 = h21 / r1
    top = c1 * h12 + s1 * h22
    low = c1 * h22 - s1 * h12
    r2 = jnp.sqrt(low * low + h32 * h32)
    c2 = low / r2
    s2 = h32 / r2
    y2 = -beta * s1 * c2 / r2
    y1 = (beta * c1 - top * y2) / r1
    weight2 = y2 * t
    final_ref[0:1] = y1 * inverse - weight2 * h11
    final_ref[1:2] = weight2
    final_ref[2:3] = beta * s1 * s2
    reduce_sent(1)


def combine(z1, z2, final, out_ref, norm_ref, buf, norm_buf, sems):
    nblk = out_ref.shape[0]
    norm_buf[...] = final[2:3]
    norm_copy = pltpu.make_async_copy(norm_buf, norm_ref, sems.at[1])
    norm_copy.start()
    for b in range(nblk):
        buf[b] = final[0:1] * z1[b] + final[1:2] * z2[b]
        pltpu.make_async_copy(buf.at[b], out_ref.at[b], sems.at[0]).start()
    pltpu.make_async_copy(buf, out_ref, sems.at[0]).wait()
    norm_copy.wait()


def in_hbm(x):
    return pltpu.with_memory_space_constraint(x, pltpu.HBM)


def on_device(sizes, schur, interface_diag, precond, load, face_blocks):
    nblk, blk = precond.shape[3:5]
    cols = load.shape[-1]
    order = schur.shape[-1]
    cap = face_blocks.shape[-1]
    slots = 6 * cap
    rows = cap * blk
    nx, ny, nz = sizes
    planes = ny * nz
    groups = cols // LANES
    vmem = pltpu.VMEM
    dma = pltpu.SemaphoreType.DMA
    hbm = pl.BlockSpec(memory_space=pltpu.HBM)
    local = pl.BlockSpec(memory_space=pltpu.VMEM)
    scalars = pl.BlockSpec(memory_space=pltpu.SMEM)
    table = face_blocks.reshape(6, cap).T
    mib = 1024 * 1024
    z1, z2, final = pl.pallas_call(
        functools.partial(kernel, sizes),
        out_shape=(
            jax.ShapeDtypeStruct((nblk, blk, cols), F32),
            jax.ShapeDtypeStruct((nblk, blk, cols), F32),
            jax.ShapeDtypeStruct((3, cols), F32),
        ),
        in_specs=[hbm] * 5,
        out_specs=(local,) * 3,
        scratch_shapes=[
            pltpu.SMEM((cap, 6), jnp.int32),
            vmem((nblk, blk, cols), BF16),
            vmem((nblk, blk, blk), F32),
            vmem((nblk, 1, blk), F32),
            vmem((nblk, nblk, blk, blk), BF16),
            vmem((slots * blk, slots * blk), BF16),
            vmem((slots * blk, LANES), F32),
            vmem((6, 2 * rows, LANES), F32),
            vmem((6, 2 * rows, LANES), F32),
            vmem((max(groups - 1, 1), 6, rows, LANES), F32),
            vmem((max(groups - 1, 1), 6, rows, LANES), F32),
            vmem((slots, blk, 2 * blk), BF16),
            vmem((groups, 6, rows, LANES), F32),
            vmem((groups, 6, rows, LANES), F32),
            vmem((groups, slots, blk, LANES), F32),
            vmem((groups, slots, blk, LANES), F32),
            vmem((groups, 6, rows, LANES), F32),
            vmem((groups, 6, rows, LANES), F32),
            vmem((groups, 6, rows, LANES), F32),
            vmem((groups, 6, rows // 2, LANES), F32),
            vmem((rows, LANES), F32),
            vmem((2 * groups - 1, rows // 2, LANES), F32),
            vmem((max(groups - 1, 1), rows // 4, LANES), F32),
            vmem((groups, 6, 8, LANES), F32),
            vmem((planes, 2 * groups, LANES), F32),
            vmem((nx, 2 * groups, LANES), F32),
            vmem((planes, 4 * groups, LANES), F32),
            vmem((nx, 4 * groups, LANES), F32),
            dma((5,)),
            dma((groups, 6)),
            dma((2 * groups, 6)),
            dma((groups,)),
            dma((2 * groups,)),
            dma((2,)),
            dma((2,)),
            dma((2,)),
            dma((2,)),
        ],
        compiler_params=pltpu.CompilerParams(
            collective_id=0, has_side_effects=True, vmem_limit_bytes=44 * mib
        ),
    )(
        in_hbm(table),
        in_hbm(schur.reshape(nblk, blk, order)),
        in_hbm(interface_diag.reshape(nblk, 1, blk)),
        in_hbm(precond.reshape(nblk, blk, blk)),
        in_hbm(load.reshape(nblk, blk, cols)),
    )
    result, norm = pl.pallas_call(
        combine,
        out_shape=(
            jax.ShapeDtypeStruct((nblk, blk, cols), F32),
            jax.ShapeDtypeStruct((1, cols), F32),
        ),
        in_specs=[local, local, local],
        out_specs=(hbm, hbm),
        scratch_shapes=[vmem((nblk, blk, cols), F32), vmem((1, cols), F32), dma((2,))],
        compiler_params=pltpu.CompilerParams(vmem_limit_bytes=16 * mib),
    )(z1, z2, final)
    return result.reshape(1, 1, 1, nblk * blk, cols), norm.reshape(cols)


def solution(mesh):
    sizes = tuple(mesh.shape[a] for a in AXES)
    placed = (
        P("gx", "gy", "gz", None, None),
        P("gx", "gy", "gz", None),
        P("gx", "gy", "gz", None, None, None),
        P("gx", "gy", "gz", None, None),
        P("gx", "gy", "gz", None, None),
    )
    return jax.shard_map(
        functools.partial(on_device, sizes),
        mesh=mesh,
        in_specs=placed,
        out_specs=(P("gx", "gy", "gz", None, None), P()),
        check_vma=False,
    )
```

```python
import functools

import jax
import jax.numpy as jnp
from jax import lax
from jax.experimental import pallas as pl
from jax.experimental.pallas import tpu as pltpu
from jax.sharding import PartitionSpec as P

EPS = 1e-06
MESH = pl.DeviceIdType.MESH
AXES = ("gx", "gy", "gz")
LANES = 128
F32 = jnp.float32
BF16 = jnp.bfloat16
NEAR = (4, 5, 0, 1)
FAR = (2, 3)
ALL = (0, 1, 2, 3, 4, 5)


def kernel(
    sizes,
    table_hbm,
    schur_hbm,
    diag_hbm,
    prec_hbm,
    load_hbm,
    z1_out,
    z2_out,
    final_ref,
    table,
    load_all,
    prec_all,
    diag_all,
    schur_all,
    schur_slots,
    diag_slots,
    first_send,
    first_recv,
    load_send,
    load_recv,
    prec_split,
    rhs,
    a_ref,
    z1_ref,
    z2_ref,
    u1_send,
    u1_recv,
    u2_send,
    u2_recv,
    pass_first,
    pass_full,
    sums,
    plane_one,
    line_one,
    plane_two,
    line_two,
    local_sems,
    face_send,
    face_recv,
    pass_send,
    pass_recv,
    plane_send,
    plane_recv,
    line_send,
    line_recv,
):
    nx, ny, nz = sizes
    planes = ny * nz
    groups, _, rows, lanes = rhs.shape
    nblk, blk = prec_hbm.shape[:2]
    cap = rows // blk
    slots = 6 * cap
    half = rows // 2
    gx, gy, gz = (lax.axis_index(a) for a in AXES)
    here = gy * nz + gz
    relayed = ny == 4 and nz == 2

    moves = [(table_hbm, table), (load_hbm, load_all), (prec_hbm, prec_all), (diag_hbm, diag_all)]
    local = [
        pltpu.make_async_copy(source, target, local_sems.at[i])
        for i, (source, target) in enumerate(moves)
    ]
    for copy in local:
        copy.start()

    def plane_peer(step):
        other = lax.rem(here + step, planes)
        return (gx, other // nz, lax.rem(other, nz))

    def line_peer(step):
        return (lax.rem(gx + step, nx), gy, gz)

    target, has = [], []
    for d in range(6):
        at = [gx, gy, gz]
        if d % 2 == 0:
            has.append(at[d // 2] + 1 < sizes[d // 2])
            at[d // 2] = at[d // 2] + 1
        else:
            has.append(at[d // 2] > 0)
            at[d // 2] = at[d // 2] - 1
        target.append(tuple(at))

    barrier = pltpu.get_barrier_semaphore()
    near = relayed and nx <= 4
    entered = jnp.int32(1)
    if near:
        for d in range(6):
            entered = entered + has[d].astype(jnp.int32)

            @pl.when(has[d])
            def _(d=d):
                pl.semaphore_signal(barrier, inc=1, device_id=target[d], device_id_type=MESH)

        pl.semaphore_signal(
            barrier, inc=1, device_id=(gx, lax.rem(gy + 2, ny), gz), device_id_type=MESH
        )
    else:
        entered = planes - 1 + nx - 1
        for step in range(1, planes):
            pl.semaphore_signal(barrier, inc=1, device_id=plane_peer(step), device_id_type=MESH)
        for step in range(1, nx):
            pl.semaphore_signal(barrier, inc=1, device_id=line_peer(step), device_id_type=MESH)

    def message(kind, g):
        if kind == "load" and g == 0:
            return g, g, first_send, first_recv, pass_first, 2 * rows, rows
        if kind == "load":
            return g, g, load_send.at[g - 1], load_recv.at[g - 1], pass_full.at[g - 1], rows, half
        if kind == "one":
            middle = pass_full.at[groups - 1 + g]
            return g, groups + g, u1_send.at[g], u1_recv.at[g], middle, rows, half
        return g, g, u2_send.at[g], u2_recv.at[g], None, rows, 0

    def before(kind, g):
        return ("load", g) if kind == "one" else None

    def ends(d):
        return (1, 3, 2) if d == 2 else (2, 0, 1)

    def face(msg, d, slot, device, row=0, size=None):
        g, number, source, landing, _, count, _ = msg
        size = size or count
        return pltpu.make_async_remote_copy(
            src_ref=source.at[d, pl.ds(row, size)],
            dst_ref=landing.at[slot, pl.ds(row, size)],
            send_sem=face_send.at[g, d],
            recv_sem=face_recv.at[number, slot],
            device_id=device,
            device_id_type=MESH,
        )

    def to_relay(msg, d):
        g, number, source, _, middle, count, via = msg
        return pltpu.make_async_remote_copy(
            src_ref=source.at[d, pl.ds(count - via, via)],
            dst_ref=middle,
            send_sem=face_send.at[g, d],
            recv_sem=pass_recv.at[number],
            device_id=(gx, ends(d)[1], gz),
            device_id_type=MESH,
        )

    def cuts(d):
        if relayed and d in FAR:
            low, high = rows // 4, rows - rows // 4
            if d == 2:
                return ((gy == 0, low), (gy == 1, half), (gy == 2, high))
            return ((gy == 1, low), (gy == 2, half), (gy == 3, high))
        return ((has[d], half),)

    def share(d, cut):
        return (cut, rows - cut) if d % 2 == 0 else (0, cut)

    def own(d, cut):
        return (0, cut) if d % 2 == 0 else (cut, rows - cut)

    def two_copy(g, d, cut):
        return face(message("two", g), d, d ^ 1, target[d], *share(d, cut))

    def two_send(g, faces):
        msg = message("two", g)
        todo = [(d, here_is, cut) for d in faces for here_is, cut in cuts(d)]
        todo.sort(key=lambda item: not (relayed and item[0] in FAR and item[2] == half))
        for d in faces:
            @pl.when(has[d])
            def _(d=d):
                sent(message("one", g), d)

        for d, here_is, cut in todo:
            @pl.when(here_is)
            def _(d=d, cut=cut):
                two_copy(g, d, cut).start()

    def two_sent(g):
        for d in range(6):
            for here_is, cut in cuts(d):
                @pl.when(here_is)
                def _(d=d, cut=cut):
                    two_copy(g, d, cut).wait_send()

    def sent(msg, d):
        face(msg, d, d ^ 1, target[d]).wait_send()

    def send_far(kind, g, begin=0, end=None):
        msg = message(kind, g)
        count, via = msg[5], msg[6]
        end = end or count
        for d in FAR:
            @pl.when(has[d])
            def _(d=d):
                if before(kind, g):
                    sent(message(*before(kind, g)), d)

        if relayed:
            for d in FAR:
                @pl.when(gy == ends(d)[0])
                def _(d=d):
                    if via and end == count:
                        to_relay(msg, d).start()
                    if begin < count - via:
                        size = min(end, count - via) - begin
                        face(msg, d, d ^ 1, target[d], begin, size).start()

        for d in FAR:
            plain = jnp.logical_and(has[d], gy != ends(d)[0]) if relayed else has[d]

            @pl.when(plain)
            def _(d=d):
                face(msg, d, d ^ 1, target[d], begin, end - begin).start()

    def send(kind, g, d):
        msg = message(kind, g)

        @pl.when(has[d])
        def _():
            if before(kind, g):
                sent(message(*before(kind, g)), d)
            face(msg, d, d ^ 1, target[d]).start()

    def forward(msg, d):
        g, number, _, landing, middle, count, via = msg
        return pltpu.make_async_remote_copy(
            src_ref=middle,
            dst_ref=landing.at[d ^ 1, pl.ds(count - via, via)],
            send_sem=pass_send.at[g],
            recv_sem=face_recv.at[number, d ^ 1],
            device_id=(gx, ends(d)[2], gz),
            device_id_type=MESH,
        )

    def relay(kind, g):
        msg = message(kind, g)
        if not relayed or not msg[6]:
            return
        for d in FAR:
            @pl.when(gy == ends(d)[1])
            def _(d=d):
                to_relay(msg, d).wait_recv()
                if before(kind, g):
                    forward(message(*before(kind, g)), d).wait_send()
                forward(msg, d).start()

    def arrived(kind, g, d):
        face(message(kind, g), d, d, target[d]).wait_recv()

    def relay_sent(msg):
        if relayed and msg[6]:
            for d in FAR:
                @pl.when(gy == ends(d)[1])
                def _(d=d):
                    forward(msg, d).wait_send()

    def plane_of(number):
        return plane_two if number else plane_one

    def line_of(number):
        return line_two if number else line_one

    def part_copy(number, buf, slot, device, send_sem, recv_sem):
        return pltpu.make_async_remote_copy(
            src_ref=buf.at[slot],
            dst_ref=buf.at[slot],
            send_sem=send_sem.at[number],
            recv_sem=recv_sem.at[number],
            device_id=device,
            device_id_type=MESH,
        )

    def parts_wait(number, count, send_sem, recv_sem, sent):
        if count:
            buf = plane_of(number)
            copy = part_copy(
                number, buf, pl.ds(0, count), line_peer(1), send_sem, recv_sem
            )
            if sent:
                copy.wait_send()
            else:
                copy.wait_recv()

    hub = nz - 1
    is_hub = gz == hub

    def reduce_start(number):
        buf = plane_of(number)
        if not relayed:
            for step in range(1, planes):
                part_copy(number, buf, here, plane_peer(step), plane_send, plane_recv).start()
            return
        for step in range(1, ny):
            device = (gx, lax.rem(gy + step, ny), hub)
            part_copy(number, buf, here, device, plane_send, plane_recv).start()

    def reduce_own(number):
        if relayed:
            @pl.when(jnp.logical_not(is_hub))
            def _():
                buf = plane_of(number)
                part_copy(number, buf, here, (gx, gy, hub), plane_send, plane_recv).start()

    def reduce_middle(number):
        line = line_of(number)
        if not relayed:
            parts_wait(number, planes - 1, plane_send, plane_recv, False)
            line[gx] = total_of(plane_of(number), planes)
            for step in range(1, nx):
                part_copy(number, line, gx, line_peer(step), line_send, line_recv).start()
            return

        @pl.when(is_hub)
        def _():
            parts_wait(number, planes - 1, plane_send, plane_recv, False)
            line[gx] = total_of(plane_of(number), planes)
            for core in range(nz):
                for step in range(1, nx):
                    device = (lax.rem(gx + nx - step, nx), gy, core)
                    part_copy(number, line, gx, device, line_send, line_recv).start()
            part_copy(number, line, gx, (gx, gy, 0), line_send, line_recv).start()

    def reduce_end(number):
        if relayed:
            for core in range(nz):
                @pl.when(gz == core)
                def _(core=core):
                    parts_wait(number, nx - (core == hub), line_send, line_recv, False)
        else:
            parts_wait(number, nx - 1, line_send, line_recv, False)
        return total_of(line_of(number), nx)

    def reduce_sent(number):
        if not relayed:
            parts_wait(number, planes - 1, plane_send, plane_recv, True)
            parts_wait(number, nx - 1, line_send, line_recv, True)
            return
        for core in range(nz):
            @pl.when(gz == core)
            def _(core=core):
                parts_wait(number, ny - (core == hub), plane_send, plane_recv, True)
                if core == hub:
                    parts_wait(number, nz * (nx - 1) + 1, line_send, line_recv, True)

    def total_of(buf, count):
        total = buf[0]
        for i in range(1, count):
            total = total + buf[i]
        return total

    def folded(x):
        return jnp.sum(x.reshape(x.shape[0] // 8, 8, lanes), axis=0)

    def add_sum(g, i, x):
        sums[g, i] = sums[g, i] + x

    local[0].wait()
    picks = [table[s % cap, s // cap] for s in range(slots)]
    index = [jnp.minimum(p, nblk - 1) for p in picks]
    mask = [jnp.minimum(nblk - p, 1).astype(F32) for p in picks]

    def gather_load(g, d):
        for k in range(cap):
            s = d * cap + k
            value = load_all[index[s], :, g * lanes : (g + 1) * lanes].astype(F32)
            if g:
                load_send[g - 1, d, k * blk : (k + 1) * blk] = value * mask[s]
            else:
                first_send[d, k * blk : (k + 1) * blk] = value * mask[s]

    def gather_prec(d):
        for k in range(cap):
            at = slice(rows + k * blk, rows + (k + 1) * blk)
            first_send[d, at] = prec_all[index[d * cap + k]]

    local[1].wait()
    for d in FAR:
        gather_load(0, d)
    pl.semaphore_wait(barrier, entered)
    send_far("load", 0, 0, rows)
    local[2].wait()
    for d in FAR:
        gather_prec(d)
    gather_load(0, 0)
    gather_prec(0)
    send_far("load", 0, rows, 2 * rows)
    gather_load(0, 1)
    gather_prec(1)
    send("load", 0, 0)
    gather_load(0, 4)
    gather_prec(4)
    send("load", 0, 1)
    gather_load(0, 5)
    gather_prec(5)
    send("load", 0, 4)
    for b in range(nblk):
        pltpu.make_async_copy(
            schur_hbm.at[:, :, pl.ds(b * blk, blk)], schur_all.at[b], local_sems.at[4]
        ).start()
    for g in range(1, groups):
        for d in range(6):
            gather_load(g, d)
    send("load", 0, 5)
    sums[...] = jnp.zeros(sums.shape, F32)
    for d in range(6):
        @pl.when(jnp.logical_not(has[d]))
        def _(d=d):
            for g in range(groups):
                blank = jnp.zeros((cap, blk, lanes), F32)
                z1_ref[g, d * cap : (d + 1) * cap] = blank
                z2_ref[g, d * cap : (d + 1) * cap] = blank

    u1_send[...] = jnp.zeros(u1_send.shape, F32)
    u2_send[...] = jnp.zeros(u2_send.shape, F32)
    local[3].wait()
    eye = lax.broadcasted_iota(jnp.int32, (blk, blk), 0) == lax.broadcasted_iota(
        jnp.int32, (blk, blk), 1
    )
    for s in range(slots):
        column = jnp.sum(jnp.where(eye, diag_all[index[s]], 0.0), axis=1, keepdims=True)
        diag_slots[s * blk : (s + 1) * blk] = jnp.broadcast_to(column, (blk, lanes))
    relay("load", 0)
    for g in range(1, groups):
        send_far("load", g)
        for d in (0, 1, 4, 5):
            send("load", g, d)
    pltpu.make_async_copy(schur_all, schur_all, local_sems.at[4]).wait()
    for s in range(slots):
        for t in range(slots):
            tile = schur_all[index[t], index[s]]
            schur_slots[s * blk : (s + 1) * blk, t * blk : (t + 1) * blk] = tile
    for g in range(1, groups):
        relay("load", g)

    def precondition(s, value):
        high = value.astype(BF16)
        low = (value - high.astype(F32)).astype(BF16)
        top = jnp.concatenate([high, low], axis=1)
        bottom = jnp.concatenate([high, jnp.zeros_like(low)], axis=1)
        z = jnp.dot(
            prec_split[s], jnp.concatenate([top, bottom], axis=0), preferred_element_type=F32
        )
        return z[:, :lanes] + z[:, lanes:]

    def narrowed(z):
        return jnp.concatenate([part.astype(BF16) for part in z], axis=0)

    def multiply(d, narrow, into, which):
        first, last = which[0], which[-1] + 1
        product = jnp.dot(
            schur_slots[first * rows : last * rows, d * rows : (d + 1) * rows],
            narrow,
            preferred_element_type=F32,
        )
        into[first:last] = into[first:last] + product.reshape(last - first, rows, lanes)

    def columns_of(z_ref, g, d):
        return narrowed([z_ref[g, d * cap + k] for k in range(cap)])

    def first_step(g, d):
        @pl.when(has[d])
        def _():
            arrived("load", g, d)
            if g == 0:
                for k in range(cap):
                    at = slice(rows + k * blk, rows + (k + 1) * blk)
                    block = first_send[d, at] + first_recv[d, at]
                    high = block.astype(BF16)
                    low = (block - high.astype(F32)).astype(BF16)
                    prec_split[d * cap + k] = jnp.concatenate([high, low], axis=1)
            z = []
            square = jnp.zeros((8, lanes), F32)
            for k in range(cap):
                at = slice(k * blk, (k + 1) * blk)
                if g:
                    value = load_send[g - 1, d, at] + load_recv[g - 1, d, at]
                else:
                    value = first_send[d, at] + first_recv[d, at]
                rhs[g, d, at] = value
                square = square + folded(value * value)
                z.append(precondition(d * cap + k, value))
                z1_ref[g, d * cap + k] = z[-1]
            add_sum(g, 0, square)
            multiply(d, narrowed(z), u1_send.at[g], ALL if d in NEAR else FAR)

    def second_step(g, d):
        @pl.when(has[d])
        def _():
            arrived("one", g, d)
            z = []
            for k in range(cap):
                s = d * cap + k
                at = slice(k * blk, (k + 1) * blk)
                value = (u1_send[g, d, at] + u1_recv[g, d, at]) * mask[s]
                a_ref[g, d, at] = value
                z.append(precondition(s, value))
                z2_ref[g, s] = z[-1]
            multiply(d, narrowed(z), u2_send.at[g], ALL if d in NEAR else FAR)

    def add_diagonal(z_ref, u_ref, g, d):
        scale = diag_slots[d * rows : (d + 1) * rows]
        u_ref[g, d] = u_ref[g, d] + scale * z_ref[g, d * cap : (d + 1) * cap].reshape(rows, lanes)

    def finish_far(g, z_ref, u_ref):
        for d in FAR:
            @pl.when(has[d])
            def _(d=d):
                add_diagonal(z_ref, u_ref, g, d)

    def finish_near(g, z_ref, u_ref):
        for d in FAR:
            @pl.when(has[d])
            def _(d=d):
                narrow = columns_of(z_ref, g, d)
                multiply(d, narrow, u_ref.at[g], (0, 1))
                multiply(d, narrow, u_ref.at[g], (4, 5))

        for d in (0, 1, 4, 5):
            @pl.when(has[d])
            def _(d=d):
                add_diagonal(z_ref, u_ref, g, d)

    def send_near(g):
        for d in (0, 1, 4, 5):
            send("one", g, d)

    def cross(g):
        for d in range(6):
            @pl.when(has[d])
            def _(d=d):
                add_sum(g, 1, folded(u1_send[g, d] * rhs[g, d]))

    def pack(values):
        return jnp.concatenate([jnp.sum(v, axis=0, keepdims=True) for v in values], axis=0)

    place = []
    for b in range(nblk):
        slot, live = jnp.int32(0), jnp.int32(0)
        for s in range(slots):
            same = 1 - jnp.minimum(jnp.abs(picks[s] - b), 1)
            slot, live = slot + s * same, live + same
        place.append((jnp.minimum(slot, slots - 1), live.astype(F32)))

    def spread(g, z_ref, z_out):
        for b in range(nblk):
            slot, live = place[b]
            z_out[b, :, g * lanes : (g + 1) * lanes] = z_ref[g, slot] * live

    last = groups - 1
    for g in range(groups):
        for d in NEAR:
            first_step(g, d)
        if g:
            relay("one", g - 1)
        for d in FAR:
            first_step(g, d)
        finish_far(g, z1_ref, u1_send)
        if g < last:
            send_far("one", g)
            finish_near(g, z1_ref, u1_send)
            send_near(g)
            cross(g)
        else:
            finish_near(g, z1_ref, u1_send)
            cross(g)
            packed = [pack((0.5 * sums[i, 0], sums[i, 1])) for i in range(groups)]
            plane_one[here] = jnp.concatenate(packed, axis=0)
            reduce_start(0)
            send_far("one", g)
            send_near(g)
        spread(g, z1_ref, z1_out)

    for g in range(groups):
        if groups == 1:
            relay("one", last)
        for d in NEAR:
            second_step(g, d)
        if g:
            two_send(g - 1, FAR)
        if g == 0:
            reduce_own(0)
            if groups > 1:
                relay("one", last)
        for d in FAR:
            second_step(g, d)
        finish_far(g, z2_ref, u2_send)
        if g == last:
            two_send(g, FAR)
        finish_near(g, z2_ref, u2_send)
        two_send(g, (0, 1, 4, 5))
        if g == 0:
            reduce_middle(0)

    def measure(g, h11):
        for d in range(6):
            @pl.when(has[d])
            def _(d=d):
                square = jnp.zeros((8, lanes), F32)
                first = jnp.zeros((8, lanes), F32)
                second = jnp.zeros((8, lanes), F32)
                for k in range(cap):
                    at = slice(k * blk, (k + 1) * blk)
                    v = rhs[g, d, at]
                    q = a_ref[g, d, at] - h11 * v
                    u = u2_send[g, d, at] - h11 * u1_send[g, d, at]
                    square = square + folded(q * q)
                    first = first + folded(u * v)
                    second = second + folded(u * q)
                add_sum(g, 2, square)
                add_sum(g, 3, first)
                add_sum(g, 4, second)

    def third_step(g, d, h11):
        for here_is, cut in cuts(d):
            @pl.when(here_is)
            def _(cut=cut):
                begin, size = own(d, cut)
                face(message("two", g), d, d, target[d], begin, size).wait_recv()
                work = jnp.zeros((8, lanes), F32)
                for k in range(cap):
                    first, last = max(begin, k * blk), min(begin + size, (k + 1) * blk)
                    if first < last:
                        at = slice(first, last)
                        w = (u2_send[g, d, at] + u2_recv[g, d, at]) * mask[d * cap + k]
                        w = w - h11 * a_ref[g, d, at]
                        work = work + folded(w * w)
                add_sum(g, 5, work)

    spread(0, z2_ref, z2_out)
    total = reduce_end(0)
    squares = [total[2 * g : 2 * g + 1] for g in range(groups)]
    inners = [total[2 * g + 1 : 2 * g + 2] / (squares[g] + EPS) for g in range(groups)]
    measure(0, inners[0])
    for g in range(1, groups):
        spread(g, z2_ref, z2_out)
        measure(g, inners[g])
    for g in range(groups):
        for d in NEAR:
            third_step(g, d, inners[g])
        for d in FAR:
            third_step(g, d, inners[g])

    packed = []
    for g in range(groups):
        packed.append(pack((0.5 * sums[g, 2], sums[g, 3], sums[g, 4], sums[g, 5])))
    plane_two[here] = jnp.concatenate(packed, axis=0)
    reduce_start(1)
    reduce_own(1)
    for g in range(groups):
        two_sent(g)
        relay_sent(message("one", g))
    reduce_sent(0)
    reduce_middle(1)
    total = reduce_end(1)

    def both(rows_of):
        return jnp.concatenate(rows_of, axis=1)

    q_square, first, second, work = (
        both([total[4 * g + i : 4 * g + i + 1] for g in range(groups)]) for i in range(4)
    )
    load_square, h11 = both(squares), both(inners)
    beta = jnp.sqrt(load_square + EPS)
    inverse = 1.0 / beta
    h21 = jnp.sqrt(q_square * inverse * inverse + EPS)
    t = inverse / h21
    h12 = first * t * inverse
    a22 = second * t * t
    ww = work * t * t
    n1 = load_square * inverse * inverse
    n2 = q_square * t * t
    g12 = h11 * EPS * inverse * t
    h22 = a22 - h12 * g12
    left = (
        ww
        - h12 * h12 * (2.0 - n1)
        - h22 * (2.0 * a22 - h22 * n2)
        + 2.0 * h12 * h22 * g12
    )
    h32 = jnp.sqrt(jnp.maximum(left, 0.0) + EPS)
    r1 = jnp.sqrt(h11 * h11 + h21 * h21)
    c1 = h11 / r1
    s1 = h21 / r1
    top = c1 * h12 + s1 * h22
    low = c1 * h22 - s1 * h12
    r2 = jnp.sqrt(low * low + h32 * h32)
    c2 = low / r2
    s2 = h32 / r2
    y2 = -beta * s1 * c2 / r2
    y1 = (beta * c1 - top * y2) / r1
    weight2 = y2 * t
    final_ref[0:1] = y1 * inverse - weight2 * h11
    final_ref[1:2] = weight2
    final_ref[2:3] = beta * s1 * s2
    reduce_sent(1)


def combine(z1, z2, final, out_ref, norm_ref, buf, norm_buf, sems):
    nblk = out_ref.shape[0]
    norm_buf[...] = final[2:3]
    norm_copy = pltpu.make_async_copy(norm_buf, norm_ref, sems.at[1])
    norm_copy.start()
    for b in range(nblk):
        buf[b] = final[0:1] * z1[b] + final[1:2] * z2[b]
        pltpu.make_async_copy(buf.at[b], out_ref.at[b], sems.at[0]).start()
    pltpu.make_async_copy(buf, out_ref, sems.at[0]).wait()
    norm_copy.wait()


def in_hbm(x):
    return pltpu.with_memory_space_constraint(x, pltpu.HBM)


def on_device(sizes, schur, interface_diag, precond, load, face_blocks):
    nblk, blk = precond.shape[3:5]
    cols = load.shape[-1]
    order = schur.shape[-1]
    cap = face_blocks.shape[-1]
    slots = 6 * cap
    rows = cap * blk
    nx, ny, nz = sizes
    planes = ny * nz
    groups = cols // LANES
    vmem = pltpu.VMEM
    dma = pltpu.SemaphoreType.DMA
    hbm = pl.BlockSpec(memory_space=pltpu.HBM)
    local = pl.BlockSpec(memory_space=pltpu.VMEM)
    scalars = pl.BlockSpec(memory_space=pltpu.SMEM)
    table = face_blocks.reshape(6, cap).T
    mib = 1024 * 1024
    z1, z2, final = pl.pallas_call(
        functools.partial(kernel, sizes),
        out_shape=(
            jax.ShapeDtypeStruct((nblk, blk, cols), F32),
            jax.ShapeDtypeStruct((nblk, blk, cols), F32),
            jax.ShapeDtypeStruct((3, cols), F32),
        ),
        in_specs=[hbm] * 5,
        out_specs=(local,) * 3,
        scratch_shapes=[
            pltpu.SMEM((cap, 6), jnp.int32),
            vmem((nblk, blk, cols), BF16),
            vmem((nblk, blk, blk), F32),
            vmem((nblk, 1, blk), F32),
            vmem((nblk, nblk, blk, blk), BF16),
            vmem((slots * blk, slots * blk), BF16),
            vmem((slots * blk, LANES), F32),
            vmem((6, 2 * rows, LANES), F32),
            vmem((6, 2 * rows, LANES), F32),
            vmem((max(groups - 1, 1), 6, rows, LANES), F32),
            vmem((max(groups - 1, 1), 6, rows, LANES), F32),
            vmem((slots, blk, 2 * blk), BF16),
            vmem((groups, 6, rows, LANES), F32),
            vmem((groups, 6, rows, LANES), F32),
            vmem((groups, slots, blk, LANES), F32),
            vmem((groups, slots, blk, LANES), F32),
            vmem((groups, 6, rows, LANES), F32),
            vmem((groups, 6, rows, LANES), F32),
            vmem((groups, 6, rows, LANES), F32),
            vmem((groups, 6, rows, LANES), F32),
            vmem((rows, LANES), F32),
            vmem((2 * groups - 1, rows // 2, LANES), F32),
            vmem((groups, 6, 8, LANES), F32),
            vmem((planes, 2 * groups, LANES), F32),
            vmem((nx, 2 * groups, LANES), F32),
            vmem((planes, 4 * groups, LANES), F32),
            vmem((nx, 4 * groups, LANES), F32),
            dma((5,)),
            dma((groups, 6)),
            dma((2 * groups, 6)),
            dma((groups,)),
            dma((2 * groups,)),
            dma((2,)),
            dma((2,)),
            dma((2,)),
            dma((2,)),
        ],
        compiler_params=pltpu.CompilerParams(
            collective_id=0, has_side_effects=True, vmem_limit_bytes=44 * mib
        ),
    )(
        in_hbm(table),
        in_hbm(schur.reshape(nblk, blk, order)),
        in_hbm(interface_diag.reshape(nblk, 1, blk)),
        in_hbm(precond.reshape(nblk, blk, blk)),
        in_hbm(load.reshape(nblk, blk, cols)),
    )
    result, norm = pl.pallas_call(
        combine,
        out_shape=(
            jax.ShapeDtypeStruct((nblk, blk, cols), F32),
            jax.ShapeDtypeStruct((1, cols), F32),
        ),
        in_specs=[local, local, local],
        out_specs=(hbm, hbm),
        scratch_shapes=[vmem((nblk, blk, cols), F32), vmem((1, cols), F32), dma((2,))],
        compiler_params=pltpu.CompilerParams(vmem_limit_bytes=16 * mib),
    )(z1, z2, final)
    return result.reshape(1, 1, 1, nblk * blk, cols), norm.reshape(cols)


def solution(mesh):
    sizes = tuple(mesh.shape[a] for a in AXES)
    placed = (
        P("gx", "gy", "gz", None, None),
        P("gx", "gy", "gz", None),
        P("gx", "gy", "gz", None, None, None),
        P("gx", "gy", "gz", None, None),
        P("gx", "gy", "gz", None, None),
    )
    return jax.shard_map(
        functools.partial(on_device, sizes),
        mesh=mesh,
        in_specs=placed,
        out_specs=(P("gx", "gy", "gz", None, None), P()),
        check_vma=False,
    )
```

```python
import functools

import jax
import jax.numpy as jnp
from jax import lax
from jax.experimental import pallas as pl
from jax.experimental.pallas import tpu as pltpu
from jax.sharding import PartitionSpec as P

EPS = 1e-06
MESH = pl.DeviceIdType.MESH
AXES = ("gx", "gy", "gz")
LANES = 128
F32 = jnp.float32
BF16 = jnp.bfloat16
NEAR = (4, 5, 0, 1)
FAR = (2, 3)
ALL = (0, 1, 2, 3, 4, 5)


def kernel(
    sizes,
    table_hbm,
    schur_hbm,
    diag_hbm,
    prec_hbm,
    load_hbm,
    z1_out,
    z2_out,
    final_ref,
    table,
    load_all,
    prec_all,
    diag_all,
    schur_all,
    schur_slots,
    diag_slots,
    first_send,
    first_recv,
    load_send,
    load_recv,
    prec_split,
    rhs,
    a_ref,
    z1_ref,
    z2_ref,
    u1_send,
    u1_recv,
    u2_send,
    u2_recv,
    pass_first,
    pass_full,
    sums,
    plane_one,
    line_one,
    plane_two,
    line_two,
    local_sems,
    face_send,
    face_recv,
    pass_send,
    pass_recv,
    plane_send,
    plane_recv,
    line_send,
    line_recv,
):
    nx, ny, nz = sizes
    planes = ny * nz
    groups, _, rows, lanes = rhs.shape
    nblk, blk = prec_hbm.shape[:2]
    cap = rows // blk
    slots = 6 * cap
    half = rows // 2
    gx, gy, gz = (lax.axis_index(a) for a in AXES)
    here = gy * nz + gz
    relayed = ny == 4 and nz == 2

    moves = [(table_hbm, table), (load_hbm, load_all), (prec_hbm, prec_all), (diag_hbm, diag_all)]
    local = [
        pltpu.make_async_copy(source, target, local_sems.at[i])
        for i, (source, target) in enumerate(moves)
    ]
    local[0].start()
    pieces = 4 if nblk % 4 == 0 else 1
    for source, goal, sem in ((load_hbm, load_all, 1), (prec_hbm, prec_all, 2)):
        for i in range(pieces):
            at = pl.ds(i * (nblk // pieces), nblk // pieces)
            pltpu.make_async_copy(source.at[at], goal.at[at], local_sems.at[sem]).start()
    local[3].start()

    def plane_peer(step):
        other = lax.rem(here + step, planes)
        return (gx, other // nz, lax.rem(other, nz))

    def line_peer(step):
        return (lax.rem(gx + step, nx), gy, gz)

    target, has = [], []
    for d in range(6):
        at = [gx, gy, gz]
        if d % 2 == 0:
            has.append(at[d // 2] + 1 < sizes[d // 2])
            at[d // 2] = at[d // 2] + 1
        else:
            has.append(at[d // 2] > 0)
            at[d // 2] = at[d // 2] - 1
        target.append(tuple(at))

    barrier = pltpu.get_barrier_semaphore()
    near = relayed and nx <= 4
    entered = jnp.int32(1)
    if near:
        for d in range(6):
            entered = entered + has[d].astype(jnp.int32)

            @pl.when(has[d])
            def _(d=d):
                pl.semaphore_signal(barrier, inc=1, device_id=target[d], device_id_type=MESH)

        pl.semaphore_signal(
            barrier, inc=1, device_id=(gx, lax.rem(gy + 2, ny), gz), device_id_type=MESH
        )
    else:
        entered = planes - 1 + nx - 1
        for step in range(1, planes):
            pl.semaphore_signal(barrier, inc=1, device_id=plane_peer(step), device_id_type=MESH)
        for step in range(1, nx):
            pl.semaphore_signal(barrier, inc=1, device_id=line_peer(step), device_id_type=MESH)

    def message(kind, g):
        if kind == "load" and g == 0:
            return g, g, first_send, first_recv, pass_first, 2 * rows, rows
        if kind == "load":
            return g, g, load_send.at[g - 1], load_recv.at[g - 1], pass_full.at[g - 1], rows, half
        if kind == "one":
            middle = pass_full.at[groups - 1 + g]
            return g, groups + g, u1_send.at[g], u1_recv.at[g], middle, rows, half
        return g, g, u2_send.at[g], u2_recv.at[g], None, rows, 0

    def before(kind, g):
        return ("load", g) if kind == "one" else None

    def sem_of(d):
        return 4 if nz == 2 and d == 5 else d

    def ends(d):
        return (1, 3, 2) if d == 2 else (2, 0, 1)

    def face(msg, d, slot, device, row=0, size=None):
        g, number, source, landing, _, count, _ = msg
        size = size or count
        return pltpu.make_async_remote_copy(
            src_ref=source.at[d, pl.ds(row, size)],
            dst_ref=landing.at[slot, pl.ds(row, size)],
            send_sem=face_send.at[g, sem_of(d)],
            recv_sem=face_recv.at[number, sem_of(slot)],
            device_id=device,
            device_id_type=MESH,
        )

    def to_relay(msg, d):
        g, number, source, _, middle, count, via = msg
        return pltpu.make_async_remote_copy(
            src_ref=source.at[d, pl.ds(count - via, via)],
            dst_ref=middle,
            send_sem=face_send.at[g, sem_of(d)],
            recv_sem=pass_recv.at[number],
            device_id=(gx, ends(d)[1], gz),
            device_id_type=MESH,
        )

    def cuts(d):
        if relayed and d in FAR:
            low, high = rows // 4, rows - rows // 4
            if d == 2:
                return ((gy == 0, low), (gy == 1, half), (gy == 2, high))
            return ((gy == 1, low), (gy == 2, half), (gy == 3, high))
        return ((has[d], half),)

    def share(d, cut):
        return (cut, rows - cut) if d % 2 == 0 else (0, cut)

    def own(d, cut):
        return (0, cut) if d % 2 == 0 else (cut, rows - cut)

    def two_copy(g, d, cut):
        return face(message("two", g), d, d ^ 1, target[d], *share(d, cut))

    def two_send(g, faces):
        msg = message("two", g)
        todo = [(d, here_is, cut) for d in faces for here_is, cut in cuts(d)]
        todo.sort(key=lambda item: not (relayed and item[0] in FAR and item[2] == half))
        for d in faces:
            @pl.when(has[d])
            def _(d=d):
                sent(message("one", g), d)

        for d, here_is, cut in todo:
            @pl.when(here_is)
            def _(d=d, cut=cut):
                two_copy(g, d, cut).start()

    def two_sent(g):
        for d in range(6):
            for here_is, cut in cuts(d):
                @pl.when(here_is)
                def _(d=d, cut=cut):
                    two_copy(g, d, cut).wait_send()

    def sent(msg, d):
        face(msg, d, d ^ 1, target[d]).wait_send()

    def send_far(kind, g, begin=0, end=None):
        msg = message(kind, g)
        count, via = msg[5], msg[6]
        end = end or count
        for d in FAR:
            @pl.when(has[d])
            def _(d=d):
                if before(kind, g):
                    sent(message(*before(kind, g)), d)

        if relayed:
            for d in FAR:
                @pl.when(gy == ends(d)[0])
                def _(d=d):
                    if via and end == count:
                        to_relay(msg, d).start()
                    if begin < count - via:
                        size = min(end, count - via) - begin
                        face(msg, d, d ^ 1, target[d], begin, size).start()

        for d in FAR:
            plain = jnp.logical_and(has[d], gy != ends(d)[0]) if relayed else has[d]

            @pl.when(plain)
            def _(d=d):
                face(msg, d, d ^ 1, target[d], begin, end - begin).start()

    def send(kind, g, d):
        msg = message(kind, g)

        @pl.when(has[d])
        def _():
            if before(kind, g):
                sent(message(*before(kind, g)), d)
            face(msg, d, d ^ 1, target[d]).start()

    def forward(msg, d):
        g, number, _, landing, middle, count, via = msg
        return pltpu.make_async_remote_copy(
            src_ref=middle,
            dst_ref=landing.at[d ^ 1, pl.ds(count - via, via)],
            send_sem=pass_send.at[g],
            recv_sem=face_recv.at[number, sem_of(d ^ 1)],
            device_id=(gx, ends(d)[2], gz),
            device_id_type=MESH,
        )

    def relay(kind, g):
        msg = message(kind, g)
        if not relayed or not msg[6]:
            return
        for d in FAR:
            @pl.when(gy == ends(d)[1])
            def _(d=d):
                to_relay(msg, d).wait_recv()
                if before(kind, g):
                    forward(message(*before(kind, g)), d).wait_send()
                forward(msg, d).start()

    def arrived(kind, g, d):
        face(message(kind, g), d, d, target[d]).wait_recv()

    def relay_sent(msg):
        if relayed and msg[6]:
            for d in FAR:
                @pl.when(gy == ends(d)[1])
                def _(d=d):
                    forward(msg, d).wait_send()

    def plane_of(number):
        return plane_two if number else plane_one

    def line_of(number):
        return line_two if number else line_one

    def part_copy(number, buf, slot, device, send_sem, recv_sem):
        return pltpu.make_async_remote_copy(
            src_ref=buf.at[slot],
            dst_ref=buf.at[slot],
            send_sem=send_sem.at[number],
            recv_sem=recv_sem.at[number],
            device_id=device,
            device_id_type=MESH,
        )

    def parts_wait(number, count, send_sem, recv_sem, sent):
        if count:
            buf = plane_of(number)
            copy = part_copy(
                number, buf, pl.ds(0, count), line_peer(1), send_sem, recv_sem
            )
            if sent:
                copy.wait_send()
            else:
                copy.wait_recv()

    hub = nz - 1
    is_hub = gz == hub

    def reduce_start(number):
        buf = plane_of(number)
        if not relayed:
            for step in range(1, planes):
                part_copy(number, buf, here, plane_peer(step), plane_send, plane_recv).start()
            return
        for step in range(1, ny):
            device = (gx, lax.rem(gy + step, ny), hub)
            part_copy(number, buf, here, device, plane_send, plane_recv).start()

    def reduce_own(number):
        if relayed:
            @pl.when(jnp.logical_not(is_hub))
            def _():
                buf = plane_of(number)
                part_copy(number, buf, here, (gx, gy, hub), plane_send, plane_recv).start()

    def reduce_middle(number):
        line = line_of(number)
        if not relayed:
            parts_wait(number, planes - 1, plane_send, plane_recv, False)
            line[gx] = total_of(plane_of(number), planes)
            for step in range(1, nx):
                part_copy(number, line, gx, line_peer(step), line_send, line_recv).start()
            return

        @pl.when(is_hub)
        def _():
            parts_wait(number, planes - 1, plane_send, plane_recv, False)
            line[gx] = total_of(plane_of(number), planes)
            for core in range(nz):
                for step in range(1, nx):
                    device = (lax.rem(gx + nx - step, nx), gy, core)
                    part_copy(number, line, gx, device, line_send, line_recv).start()
            part_copy(number, line, gx, (gx, gy, 0), line_send, line_recv).start()

    def reduce_end(number):
        if relayed:
            for core in range(nz):
                @pl.when(gz == core)
                def _(core=core):
                    parts_wait(number, nx - (core == hub), line_send, line_recv, False)
        else:
            parts_wait(number, nx - 1, line_send, line_recv, False)
        return total_of(line_of(number), nx)

    def reduce_sent(number):
        if not relayed:
            parts_wait(number, planes - 1, plane_send, plane_recv, True)
            parts_wait(number, nx - 1, line_send, line_recv, True)
            return
        for core in range(nz):
            @pl.when(gz == core)
            def _(core=core):
                parts_wait(number, ny - (core == hub), plane_send, plane_recv, True)
                if core == hub:
                    parts_wait(number, nz * (nx - 1) + 1, line_send, line_recv, True)

    def total_of(buf, count):
        total = buf[0]
        for i in range(1, count):
            total = total + buf[i]
        return total

    def folded(x):
        return jnp.sum(x.reshape(x.shape[0] // 8, 8, lanes), axis=0)

    def add_sum(g, i, x):
        sums[g, i] = sums[g, i] + x

    local[0].wait()
    picks = [table[s % cap, s // cap] for s in range(slots)]
    index = [jnp.minimum(p, nblk - 1) for p in picks]
    mask = [jnp.minimum(nblk - p, 1).astype(F32) for p in picks]

    def gather_load(g, d):
        for k in range(cap):
            s = d * cap + k
            value = load_all[index[s], :, g * lanes : (g + 1) * lanes].astype(F32)
            if g:
                load_send[g - 1, d, k * blk : (k + 1) * blk] = value * mask[s]
            else:
                first_send[d, k * blk : (k + 1) * blk] = value * mask[s]

    def gather_prec(d):
        for k in range(cap):
            at = slice(rows + k * blk, rows + (k + 1) * blk)
            first_send[d, at] = prec_all[index[d * cap + k]]

    local[1].wait()
    for d in FAR:
        gather_load(0, d)
    pl.semaphore_wait(barrier, entered)
    send_far("load", 0, 0, rows)
    local[2].wait()
    for d in FAR:
        gather_prec(d)
    gather_load(0, 0)
    gather_prec(0)
    send_far("load", 0, rows, 2 * rows)
    gather_load(0, 1)
    gather_prec(1)
    send("load", 0, 0)
    gather_load(0, 4)
    gather_prec(4)
    send("load", 0, 1)
    gather_load(0, 5)
    gather_prec(5)
    send("load", 0, 4)
    for b in range(nblk):
        pltpu.make_async_copy(
            schur_hbm.at[:, :, pl.ds(b * blk, blk)], schur_all.at[b], local_sems.at[4]
        ).start()
    for g in range(1, groups):
        for d in range(6):
            gather_load(g, d)
    send("load", 0, 5)
    sums[...] = jnp.zeros(sums.shape, F32)
    for d in range(6):
        @pl.when(jnp.logical_not(has[d]))
        def _(d=d):
            for g in range(groups):
                blank = jnp.zeros((cap, blk, lanes), F32)
                z1_ref[g, d * cap : (d + 1) * cap] = blank
                z2_ref[g, d * cap : (d + 1) * cap] = blank

    u1_send[...] = jnp.zeros(u1_send.shape, F32)
    u2_send[...] = jnp.zeros(u2_send.shape, F32)
    local[3].wait()
    eye = lax.broadcasted_iota(jnp.int32, (blk, blk), 0) == lax.broadcasted_iota(
        jnp.int32, (blk, blk), 1
    )
    for s in range(slots):
        column = jnp.sum(jnp.where(eye, diag_all[index[s]], 0.0), axis=1, keepdims=True)
        diag_slots[s * blk : (s + 1) * blk] = jnp.broadcast_to(column, (blk, lanes))
    relay("load", 0)
    for g in range(1, groups):
        send_far("load", g)
        for d in (0, 1, 4, 5):
            send("load", g, d)
    pltpu.make_async_copy(schur_all, schur_all, local_sems.at[4]).wait()
    for s in range(slots):
        for t in range(slots):
            tile = schur_all[index[t], index[s]]
            schur_slots[s * blk : (s + 1) * blk, t * blk : (t + 1) * blk] = tile
    for g in range(1, groups):
        relay("load", g)

    def precondition(s, value):
        high = value.astype(BF16)
        low = (value - high.astype(F32)).astype(BF16)
        top = jnp.concatenate([high, low], axis=1)
        bottom = jnp.concatenate([high, jnp.zeros_like(low)], axis=1)
        z = jnp.dot(
            prec_split[s], jnp.concatenate([top, bottom], axis=0), preferred_element_type=F32
        )
        return z[:, :lanes] + z[:, lanes:]

    def narrowed(z):
        return jnp.concatenate([part.astype(BF16) for part in z], axis=0)

    def multiply(d, narrow, into, which):
        first, last = which[0], which[-1] + 1
        product = jnp.dot(
            schur_slots[first * rows : last * rows, d * rows : (d + 1) * rows],
            narrow,
            preferred_element_type=F32,
        )
        into[first:last] = into[first:last] + product.reshape(last - first, rows, lanes)

    def columns_of(z_ref, g, d):
        return narrowed([z_ref[g, d * cap + k] for k in range(cap)])

    def far_steps(step, g):
        if not relayed:
            for d in FAR:
                step(g, d, has[d], FAR)
            return
        step(g, 3, gy == 1, ALL)
        step(g, 2, gy == 2, ALL)
        step(g, 2, gy <= 1, FAR)
        step(g, 3, gy >= 2, FAR)

    late = ((2, gy <= 1), (3, gy >= 2)) if relayed else tuple((d, has[d]) for d in FAR)

    def first_step(g, d, here_is, which):
        @pl.when(here_is)
        def _():
            arrived("load", g, d)
            if g == 0:
                for k in range(cap):
                    at = slice(rows + k * blk, rows + (k + 1) * blk)
                    block = first_send[d, at] + first_recv[d, at]
                    high = block.astype(BF16)
                    low = (block - high.astype(F32)).astype(BF16)
                    prec_split[d * cap + k] = jnp.concatenate([high, low], axis=1)
            z = []
            square = jnp.zeros((8, lanes), F32)
            for k in range(cap):
                at = slice(k * blk, (k + 1) * blk)
                if g:
                    value = load_send[g - 1, d, at] + load_recv[g - 1, d, at]
                else:
                    value = first_send[d, at] + first_recv[d, at]
                rhs[g, d, at] = value
                square = square + folded(value * value)
                z.append(precondition(d * cap + k, value))
                z1_ref[g, d * cap + k] = z[-1]
            add_sum(g, 0, square)
            multiply(d, narrowed(z), u1_send.at[g], which)

    def second_step(g, d, here_is, which):
        @pl.when(here_is)
        def _():
            arrived("one", g, d)
            z = []
            for k in range(cap):
                s = d * cap + k
                at = slice(k * blk, (k + 1) * blk)
                value = (u1_send[g, d, at] + u1_recv[g, d, at]) * mask[s]
                a_ref[g, d, at] = value
                z.append(precondition(s, value))
                z2_ref[g, s] = z[-1]
            multiply(d, narrowed(z), u2_send.at[g], which)

    def add_diagonal(z_ref, u_ref, g, d):
        scale = diag_slots[d * rows : (d + 1) * rows]
        u_ref[g, d] = u_ref[g, d] + scale * z_ref[g, d * cap : (d + 1) * cap].reshape(rows, lanes)

    def finish_far(g, z_ref, u_ref):
        for d in FAR:
            @pl.when(has[d])
            def _(d=d):
                add_diagonal(z_ref, u_ref, g, d)

    def finish_near(g, z_ref, u_ref):
        for d, here_is in late:
            @pl.when(here_is)
            def _(d=d):
                narrow = columns_of(z_ref, g, d)
                multiply(d, narrow, u_ref.at[g], (0, 1))
                multiply(d, narrow, u_ref.at[g], (4, 5))

        for d in (0, 1, 4, 5):
            @pl.when(has[d])
            def _(d=d):
                add_diagonal(z_ref, u_ref, g, d)

    def send_near(g):
        for d in (0, 1, 4, 5):
            send("one", g, d)

    def cross(g):
        for d in range(6):
            @pl.when(has[d])
            def _(d=d):
                add_sum(g, 1, folded(u1_send[g, d] * rhs[g, d]))

    def pack(values):
        return jnp.concatenate([jnp.sum(v, axis=0, keepdims=True) for v in values], axis=0)

    place = []
    for b in range(nblk):
        slot, live = jnp.int32(0), jnp.int32(0)
        for s in range(slots):
            same = 1 - jnp.minimum(jnp.abs(picks[s] - b), 1)
            slot, live = slot + s * same, live + same
        place.append((jnp.minimum(slot, slots - 1), live.astype(F32)))

    def spread(g, z_ref, z_out):
        for b in range(nblk):
            slot, live = place[b]
            z_out[b, :, g * lanes : (g + 1) * lanes] = z_ref[g, slot] * live

    last = groups - 1
    for g in range(groups):
        for d in NEAR:
            first_step(g, d, has[d], ALL)
        if g:
            relay("one", g - 1)
        far_steps(first_step, g)
        finish_far(g, z1_ref, u1_send)
        if g < last:
            send_far("one", g)
            finish_near(g, z1_ref, u1_send)
            send_near(g)
            cross(g)
        else:
            finish_near(g, z1_ref, u1_send)
            cross(g)
            packed = [pack((0.5 * sums[i, 0], sums[i, 1])) for i in range(groups)]
            plane_one[here] = jnp.concatenate(packed, axis=0)
            reduce_start(0)
            send_far("one", g)
            send_near(g)
        spread(g, z1_ref, z1_out)

    for g in range(groups):
        if groups == 1:
            relay("one", last)
        for d in NEAR:
            second_step(g, d, has[d], ALL)
        if g:
            two_send(g - 1, FAR)
        if g == 0:
            reduce_own(0)
            if groups > 1:
                relay("one", last)
        far_steps(second_step, g)
        finish_far(g, z2_ref, u2_send)
        if g == last:
            two_send(g, FAR)
        finish_near(g, z2_ref, u2_send)
        two_send(g, (0, 1, 4, 5))
        if g == 0:
            reduce_middle(0)

    def measure(g, h11):
        for d in range(6):
            @pl.when(has[d])
            def _(d=d):
                square = jnp.zeros((8, lanes), F32)
                first = jnp.zeros((8, lanes), F32)
                second = jnp.zeros((8, lanes), F32)
                for k in range(cap):
                    at = slice(k * blk, (k + 1) * blk)
                    v = rhs[g, d, at]
                    q = a_ref[g, d, at] - h11 * v
                    u = u2_send[g, d, at] - h11 * u1_send[g, d, at]
                    square = square + folded(q * q)
                    first = first + folded(u * v)
                    second = second + folded(u * q)
                add_sum(g, 2, square)
                add_sum(g, 3, first)
                add_sum(g, 4, second)

    def third_step(g, d, h11):
        for here_is, cut in cuts(d):
            @pl.when(here_is)
            def _(cut=cut):
                begin, size = own(d, cut)
                face(message("two", g), d, d, target[d], begin, size).wait_recv()
                work = jnp.zeros((8, lanes), F32)
                for k in range(cap):
                    first, last = max(begin, k * blk), min(begin + size, (k + 1) * blk)
                    if first < last:
                        at = slice(first, last)
                        w = (u2_send[g, d, at] + u2_recv[g, d, at]) * mask[d * cap + k]
                        w = w - h11 * a_ref[g, d, at]
                        work = work + folded(w * w)
                add_sum(g, 5, work)

    spread(0, z2_ref, z2_out)
    total = reduce_end(0)
    squares = [total[2 * g : 2 * g + 1] for g in range(groups)]
    inners = [total[2 * g + 1 : 2 * g + 2] / (squares[g] + EPS) for g in range(groups)]
    measure(0, inners[0])
    for g in range(1, groups):
        spread(g, z2_ref, z2_out)
        measure(g, inners[g])
    for g in range(groups):
        for d in NEAR:
            third_step(g, d, inners[g])
        for d in FAR:
            third_step(g, d, inners[g])

    packed = []
    for g in range(groups):
        packed.append(pack((0.5 * sums[g, 2], sums[g, 3], sums[g, 4], sums[g, 5])))
    plane_two[here] = jnp.concatenate(packed, axis=0)
    reduce_start(1)
    reduce_own(1)
    for g in range(groups):
        two_sent(g)
        relay_sent(message("one", g))
    reduce_sent(0)
    reduce_middle(1)
    total = reduce_end(1)

    def both(rows_of):
        return jnp.concatenate(rows_of, axis=1)

    q_square, first, second, work = (
        both([total[4 * g + i : 4 * g + i + 1] for g in range(groups)]) for i in range(4)
    )
    load_square, h11 = both(squares), both(inners)
    beta = jnp.sqrt(load_square + EPS)
    inverse = 1.0 / beta
    h21 = jnp.sqrt(q_square * inverse * inverse + EPS)
    t = inverse / h21
    h12 = first * t * inverse
    a22 = second * t * t
    ww = work * t * t
    n1 = load_square * inverse * inverse
    n2 = q_square * t * t
    g12 = h11 * EPS * inverse * t
    h22 = a22 - h12 * g12
    left = (
        ww
        - h12 * h12 * (2.0 - n1)
        - h22 * (2.0 * a22 - h22 * n2)
        + 2.0 * h12 * h22 * g12
    )
    h32 = jnp.sqrt(jnp.maximum(left, 0.0) + EPS)
    r1 = jnp.sqrt(h11 * h11 + h21 * h21)
    c1 = h11 / r1
    s1 = h21 / r1
    top = c1 * h12 + s1 * h22
    low = c1 * h22 - s1 * h12
    r2 = jnp.sqrt(low * low + h32 * h32)
    c2 = low / r2
    s2 = h32 / r2
    y2 = -beta * s1 * c2 / r2
    y1 = (beta * c1 - top * y2) / r1
    weight2 = y2 * t
    final_ref[0:1] = y1 * inverse - weight2 * h11
    final_ref[1:2] = weight2
    final_ref[2:3] = beta * s1 * s2
    reduce_sent(1)


def combine(z1, z2, final, out_ref, norm_ref, buf, norm_buf, sems):
    nblk = out_ref.shape[0]
    norm_buf[...] = final[2:3]
    norm_copy = pltpu.make_async_copy(norm_buf, norm_ref, sems.at[1])
    norm_copy.start()
    for b in range(nblk):
        buf[b] = final[0:1] * z1[b] + final[1:2] * z2[b]
        pltpu.make_async_copy(buf.at[b], out_ref.at[b], sems.at[0]).start()
    pltpu.make_async_copy(buf, out_ref, sems.at[0]).wait()
    norm_copy.wait()


def in_hbm(x):
    return pltpu.with_memory_space_constraint(x, pltpu.HBM)


def on_device(sizes, schur, interface_diag, precond, load, face_blocks):
    nblk, blk = precond.shape[3:5]
    cols = load.shape[-1]
    order = schur.shape[-1]
    cap = face_blocks.shape[-1]
    slots = 6 * cap
    rows = cap * blk
    nx, ny, nz = sizes
    planes = ny * nz
    groups = cols // LANES
    vmem = pltpu.VMEM
    dma = pltpu.SemaphoreType.DMA
    hbm = pl.BlockSpec(memory_space=pltpu.HBM)
    local = pl.BlockSpec(memory_space=pltpu.VMEM)
    scalars = pl.BlockSpec(memory_space=pltpu.SMEM)
    table = face_blocks.reshape(6, cap).T
    mib = 1024 * 1024
    z1, z2, final = pl.pallas_call(
        functools.partial(kernel, sizes),
        out_shape=(
            jax.ShapeDtypeStruct((nblk, blk, cols), F32),
            jax.ShapeDtypeStruct((nblk, blk, cols), F32),
            jax.ShapeDtypeStruct((3, cols), F32),
        ),
        in_specs=[hbm] * 5,
        out_specs=(local,) * 3,
        scratch_shapes=[
            pltpu.SMEM((cap, 6), jnp.int32),
            vmem((nblk, blk, cols), BF16),
            vmem((nblk, blk, blk), F32),
            vmem((nblk, 1, blk), F32),
            vmem((nblk, nblk, blk, blk), BF16),
            vmem((slots * blk, slots * blk), BF16),
            vmem((slots * blk, LANES), F32),
            vmem((6, 2 * rows, LANES), F32),
            vmem((6, 2 * rows, LANES), F32),
            vmem((max(groups - 1, 1), 6, rows, LANES), F32),
            vmem((max(groups - 1, 1), 6, rows, LANES), F32),
            vmem((slots, blk, 2 * blk), BF16),
            vmem((groups, 6, rows, LANES), F32),
            vmem((groups, 6, rows, LANES), F32),
            vmem((groups, slots, blk, LANES), F32),
            vmem((groups, slots, blk, LANES), F32),
            vmem((groups, 6, rows, LANES), F32),
            vmem((groups, 6, rows, LANES), F32),
            vmem((groups, 6, rows, LANES), F32),
            vmem((groups, 6, rows, LANES), F32),
            vmem((rows, LANES), F32),
            vmem((2 * groups - 1, rows // 2, LANES), F32),
            vmem((groups, 6, 8, LANES), F32),
            vmem((planes, 2 * groups, LANES), F32),
            vmem((nx, 2 * groups, LANES), F32),
            vmem((planes, 4 * groups, LANES), F32),
            vmem((nx, 4 * groups, LANES), F32),
            dma((5,)),
            dma((groups, 5 if nz == 2 else 6)),
            dma((2 * groups, 5 if nz == 2 else 6)),
            dma((groups,)),
            dma((2 * groups,)),
            dma((2,)),
            dma((2,)),
            dma((2,)),
            dma((2,)),
        ],
        compiler_params=pltpu.CompilerParams(
            collective_id=0, has_side_effects=True, vmem_limit_bytes=44 * mib
        ),
    )(
        in_hbm(table),
        in_hbm(schur.reshape(nblk, blk, order)),
        in_hbm(interface_diag.reshape(nblk, 1, blk)),
        in_hbm(precond.reshape(nblk, blk, blk)),
        in_hbm(load.reshape(nblk, blk, cols)),
    )
    result, norm = pl.pallas_call(
        combine,
        out_shape=(
            jax.ShapeDtypeStruct((nblk, blk, cols), F32),
            jax.ShapeDtypeStruct((1, cols), F32),
        ),
        in_specs=[local, local, local],
        out_specs=(hbm, hbm),
        scratch_shapes=[vmem((nblk, blk, cols), F32), vmem((1, cols), F32), dma((2,))],
        compiler_params=pltpu.CompilerParams(vmem_limit_bytes=16 * mib),
    )(z1, z2, final)
    return result.reshape(1, 1, 1, nblk * blk, cols), norm.reshape(cols)


def solution(mesh):
    sizes = tuple(mesh.shape[a] for a in AXES)
    placed = (
        P("gx", "gy", "gz", None, None),
        P("gx", "gy", "gz", None),
        P("gx", "gy", "gz", None, None, None),
        P("gx", "gy", "gz", None, None),
        P("gx", "gy", "gz", None, None),
    )
    return jax.shard_map(
        functools.partial(on_device, sizes),
        mesh=mesh,
        in_specs=placed,
        out_specs=(P("gx", "gy", "gz", None, None), P()),
        check_vma=False,
    )
```
